16 devices in a mesh: dp: 2 (over y, z), tp: 8 (over x, core).
Axes of the slice: x: 4, y: 2, z: 1, core: 2. Of those that a mesh axis runs over, the one named last changes fastest.
The devices are a block of a 4x4x8 slice.
Arguments:
- x: bfloat16 [6144, 3072], P(('dp', 'tp')), parts along dimension 0
- dy: bfloat16 [6144, 3072], P(('dp', 'tp')), parts along dimension 0
- gain: bfloat16 [3072], replicated
- wq: bfloat16 [3072, 3072], P(None, 'tp')
- wk: bfloat16 [3072, 1024], P(None, 'tp')
- wv: bfloat16 [3072, 1024], P(None, 'tp')
- wo: bfloat16 [3072, 3072], P('tp')
Outputs:
- output 1: bfloat16 [6144, 3072], P(('dp', 'tp')), parts along dimension 0
- output 2: float32 [2, 3072], P('dp'), parts along dimension 0
- output 3: bfloat16 [6144, 3072], P('dp', 'tp'), parts along dimension 0
- output 4: bfloat16 [6144, 1024], P('dp', 'tp'), parts along dimension 0
- output 5: bfloat16 [6144, 1024], P('dp', 'tp'), parts along dimension 0
- output 6: bfloat16 [6144, 3072], P(('dp', 'tp')), parts along dimension 0
There are 2 independent parts. The reference program is written for one: setup_inputs(seed, part) draws one part's arguments, and reference() takes and returns one part's arrays. A program takes and returns all parts, laid end to end along the dimension named above; an argument that names none is the same for every part.
All inputs are finite; a program needn't handle non-finite values.
Results may differ from the reference program's by a relative error of at most 0.018.
Values are sent between devices in bfloat16 or wider.
A program may use at most 768 MiB of HBM per device.

```python
import jax
import jax.numpy as jnp
from jax import lax

ROWS = 3072
D = 3072
HEADS = 24
KV_HEADS = 8
HEAD = 128
THETA = 10000


def setup_inputs(seed: int = 0, part: int = 0) -> dict:
    kx, ky, kn, kq, kk, kv, ko = jax.random.split(jax.random.key(seed), 7)

    def weights(key, rows, columns):
        return jax.random.normal(key, (rows, columns), jnp.float32) * rows**-0.5

    drawn = {
        "x": jax.random.normal(jax.random.fold_in(kx, part), (ROWS, D), jnp.float32),
        "dy": jax.random.normal(jax.random.fold_in(ky, part), (ROWS, D), jnp.float32) * ROWS**-0.5,
        "gain": 1 + 0.1 * jax.random.normal(kn, (D,), jnp.float32),
        "wq": 2 * weights(kq, D, HEADS * HEAD),
        "wk": 2 * weights(kk, D, KV_HEADS * HEAD),
        "wv": 4 * weights(kv, D, KV_HEADS * HEAD),
        "wo": weights(ko, HEADS * HEAD, D),
    }
    return {k: v.astype(jnp.bfloat16) for k, v in drawn.items()}


def normed(x, gain):
    wide = x.astype(jnp.float32)
    scale = lax.rsqrt(jnp.mean(wide * wide, -1, keepdims=True) + 1e-6)
    return (wide * scale * gain.astype(jnp.float32)).astype(jnp.bfloat16)


def turned(t, place, theta):
    half = t.shape[-1] // 2
    angle = place.astype(jnp.float32)[:, None] * theta ** (-jnp.arange(half, dtype=jnp.float32) / half)
    cos, sin = jnp.cos(angle)[:, None], jnp.sin(angle)[:, None]
    a, b = t[..., :half].astype(jnp.float32), t[..., half:].astype(jnp.float32)
    return jnp.concatenate([a * cos - b * sin, b * cos + a * sin], -1).astype(jnp.bfloat16)


def matmul(a, w):
    return jnp.dot(a, w, preferred_element_type=jnp.float32).astype(jnp.bfloat16)


def einsum(form, a, b):
    return jnp.einsum(form, a.astype(jnp.float32), b.astype(jnp.float32))


def attention(q, k, v):
    scores = einsum("tgsd,ugd->gstu", q, k) * q.shape[-1] ** -0.5
    token = jnp.arange(q.shape[0])
    scores = jnp.where(token[:, None] >= token, scores, -jnp.inf)
    weights = jax.nn.softmax(scores, -1).astype(jnp.bfloat16)
    return einsum("gstu,ugd->tgsd", weights, v).astype(jnp.bfloat16)


def forward(x, gain, wq, wk, wv, wo):
    rows = x.shape[0]
    a, place = normed(x, gain), jnp.arange(rows)
    k = turned(matmul(a, wk).reshape(rows, -1, HEAD), place, THETA)
    q = turned(matmul(a, wq).reshape(rows, -1, HEAD), place, THETA).reshape(rows, k.shape[1], -1, HEAD)
    v = matmul(a, wv).reshape(rows, -1, HEAD)
    seen = attention(q, k, v).reshape(rows, -1)
    return (x.astype(jnp.float32) + jnp.dot(seen, wo, preferred_element_type=jnp.float32)).astype(jnp.bfloat16)


def reference(x, dy, gain, wq, wk, wv, wo):
    _, back = jax.vjp(forward, x, gain.astype(jnp.float32), wq, wk, wv, wo)
    by_x, by_gain, *by_weights = back(dy)
    return (by_x, by_gain[None], *by_weights)
```

```python
import functools

import jax
import jax.numpy as jnp
import numpy as np
from jax import lax
from jax.experimental import pallas as pl
from jax.experimental.pallas import tpu as pltpu
from jax.sharding import PartitionSpec as P

HEAD = 128
THETA = 10000
NEG = -1e30
HIDDEN = 2 * NEG
LOG2E = 1.4426950408889634
VMEM = 67_043_328
MESH = pl.DeviceIdType.MESH
F32, LOW = jnp.float32, jnp.bfloat16


def _dot(a, b, ca, cb):
    return lax.dot_general(a, b, (((ca,), (cb,)), ((), ())), preferred_element_type=F32)


def _at(start, size):
    return pl.ds(pl.multiple_of(start, size), size)


def _places(n):
    me = lax.axis_index("tp")
    core = lax.rem(me, 2)
    turn = 1 - 2 * core
    return me, core, turn, lax.rem(me + 2, n), lax.rem(me + n - 2, n), lax.rem(me + n // 2, n)


def _greet(devices):
    barrier = pltpu.get_barrier_semaphore()
    for d in devices:
        pl.semaphore_signal(barrier, inc=1, device_id={"tp": d}, device_id_type=MESH)
    pl.semaphore_wait(barrier, len(devices))


def _front(n, heads, x_ref, dy_ref, gain_ref, wq_ref, wk_ref, wv_ref, wo_ref, near_ref, far_ref, a_ref, g_ref, seen_ref, grads_ref,
           chunk_s, w_s, wo_s, q_s, k_s, kt_s, v_s, vt_s, lse_s, do_s, top_s, mix_s, dq_s, dk_s, dv_s, send, recv, loc):
    tok, dim = x_ref.shape
    half, hw = tok // 2, heads * HEAD
    me, core, turn, right, left, across = _places(n)
    other = me + turn
    e = HEAD**-0.5 * LOG2E

    def rows(dev, part=None):
        return _at(dev * tok, tok) if part is None else _at(dev * tok + part * half, half)

    sent = [(me, 0), (me, 1), (left, 0), (me, 1), (me, 0), (right, 1),
            (me, None), (left, 0), (right, 1), (left, 1), (right, 0), (across, 0), (across, 1)]
    got = [(left, 0), (left, 1), (across, 0), (right, 1), (right, 0), (across, 1)] + [(d + turn, h) for d, h in sent[6:]]
    to = [right] * 3 + [left] * 3 + [other] * 7

    def copy(z, i, what, src=None):
        full = a_ref if z == 0 else g_ref
        at = rows(*what)
        return pltpu.make_async_remote_copy(
            src_ref=full.at[at] if src is None else src, dst_ref=full.at[at], send_sem=send.at[z, i], recv_sem=recv.at[z, i],
            device_id={"tp": to[i]}, device_id_type=MESH)

    def start(z, *pieces):
        for i in pieces:
            own = z == 1 and i in (0, 1, 3, 4, 6)
            src = None
            if own:
                part = sent[i][1]
                src = dy_ref if part is None else dy_ref.at[pl.ds(part * half, half)]
            copy(z, i, sent[i], src).start()

    def arrived(z, *pieces):
        for i in pieces:
            copy(z, i, got[i]).wait_recv()

    def order(s):
        g = s // 2
        chip = lax.rem(me // 2 + g + g // 2 - 2 * (g // 3), n // 2)
        return chip * 2 + lax.rem(core + s, 2)

    load_x = pltpu.make_async_copy(x_ref, chunk_s.at[0], loc.at[0])
    load_x.start()
    loads = [pltpu.make_async_copy(wq_ref, w_s.at[:, :hw], loc.at[1]),
             pltpu.make_async_copy(wk_ref, w_s.at[:, hw:hw + HEAD], loc.at[2]),
             pltpu.make_async_copy(wv_ref, w_s.at[:, hw + HEAD:], loc.at[3])]
    for load in loads:
        load.start()
    load_wo = pltpu.make_async_copy(wo_ref, wo_s, loc.at[4])
    load_wo.start()
    _greet([left, right, other])

    load_x.wait()
    block = 32

    def norm(r, _):
        at = _at(r * block, block)
        wide = chunk_s[0, at, :].astype(F32)
        scale = lax.rsqrt(jnp.mean(wide * wide, -1, keepdims=True) + 1e-6)
        chunk_s[0, at, :] = (wide * scale * gain_ref[...].astype(F32)).astype(LOW)

    lax.fori_loop(0, tok // block, norm, None)
    keep = pltpu.make_async_copy(chunk_s.at[0], a_ref.at[rows(me)], loc.at[0])
    keep.start()
    keep.wait()
    start(0, 0, 3, 1, 4, 6)
    for load in loads:
        load.wait()

    def tables(j):
        ca, sa = near_ref[0], near_ref[1]
        cb, sb = far_ref[0, pl.ds(j, 1), :], far_ref[1, pl.ds(j, 1), :]
        return ca * cb - sa * sb, sa * cb + ca * sb

    def turned(t, cos, sin):
        return (t * cos + pltpu.roll(t, HEAD // 2, 1) * sin).astype(LOW)

    def project(j, slot):
        y = _dot(chunk_s[slot], w_s[...], 1, 0).astype(LOW).astype(F32)
        cos, sin = tables(j)
        for h in range(heads):
            q_s[j, h * tok:(h + 1) * tok, :] = turned(y[:, h * HEAD:(h + 1) * HEAD], cos, sin)
        at = rows(j)
        k = turned(y[:, hw:hw + HEAD], cos, sin)
        v = y[:, hw + HEAD:].astype(LOW)
        k_s[at, :] = k
        kt_s[:, at] = k.T
        v_s[at, :] = v
        vt_s[:HEAD, at] = v.T

    vt_s[HEAD:, :] = jnp.ones((8, n * tok), LOW)

    def x_step(s, _):
        j = order(s)

        @pl.when(s == 1)
        def _():
            arrived(0, 6)

        @pl.when(s == 2)
        def _():
            arrived(0, 0, 3)
            start(0, 2, 5, 7, 8)
            arrived(0, 1, 4)
            start(0, 9, 10)
            start(1, 0, 3, 1, 4, 6)

        @pl.when(s == 3)
        def _():
            arrived(0, 7, 8, 9, 10)

        @pl.when(s == 6)
        def _():
            arrived(0, 2, 5)
            start(0, 11, 12)

        @pl.when(s == 7)
        def _():
            arrived(0, 11, 12)

        @pl.when(s > 0)
        def _():
            load = pltpu.make_async_copy(a_ref.at[rows(j)], chunk_s.at[0], loc.at[0])
            load.start()
            load.wait()

        project(j, 0)

    lax.fori_loop(0, n, x_step, None)

    cols = heads * tok
    strips = [pl.ds(h * tok, tok) for h in range(heads)]

    def visible():
        return lax.broadcasted_iota(jnp.int32, (tok, tok), 1) >= lax.broadcasted_iota(jnp.int32, (tok, tok), 0)

    def forward(j, _):
        top_s[...] = jnp.full((1, cols), NEG, F32)
        mix_s[...] = jnp.zeros((HEAD + 8, cols), F32)

        def block(i, masked):
            here = rows(i)
            scores = [_dot(k_s[here, :], q_s[j, at, :], 1, 1) for at in strips]
            weights, keeps = [], []
            for at, s in zip(strips, scores):
                if masked:
                    s = jnp.where(visible(), s, HIDDEN)
                old = top_s[:, at]
                top = jnp.maximum(old, s.max(axis=0, keepdims=True))
                top_s[:, at] = top
                weights.append(jnp.exp2((s - top) * e).astype(LOW))
                keeps.append(jnp.exp2((old - top) * e))
            for at, p, kept in zip(strips, weights, keeps):
                mix_s[:, at] = mix_s[:, at] * kept + _dot(vt_s[:, here], p, 1, 0)

        lax.fori_loop(0, j, lambda i, _: block(i, False), None)
        block(j, True)
        total = mix_s[HEAD:HEAD + 1, :]
        out = (mix_s[:HEAD, :] * (1 / total)).T.astype(LOW)
        for h in range(heads):
            seen_ref[rows(j), h * HEAD:(h + 1) * HEAD] = out[h * tok:(h + 1) * tok]
        lse_s[j] = top_s[...] * e + jnp.log2(total)

    lax.fori_loop(0, n, forward, None)

    load_wo.wait()
    dk_s[...] = jnp.zeros_like(dk_s)
    dv_s[...] = jnp.zeros_like(dv_s)

    def g_load(s, src=None):
        return pltpu.make_async_copy(g_ref.at[rows(order(s))] if src is None else src, chunk_s.at[lax.rem(s, 2)], loc.at[lax.rem(s, 2)])

    def next_load(s):
        @pl.when(s == 1)
        def _():
            arrived(1, 6)

        @pl.when(s == 2)
        def _():
            arrived(1, 1, 4)
            start(1, 9, 10)

        @pl.when(s == 3)
        def _():
            arrived(1, 7, 8, 9, 10)

        @pl.when(s == 6)
        def _():
            arrived(1, 2, 5)
            start(1, 11, 12)

        @pl.when(s == 7)
        def _():
            arrived(1, 11, 12)

        @pl.when(s < n)
        def _():
            g_load(s).start()

    arrived(1, 0, 3)
    start(1, 2, 5, 7, 8)
    first = pltpu.make_async_copy(dy_ref, chunk_s.at[0], loc.at[0])
    first.start()

    def backward(s, _):
        j = order(s)
        slot = lax.rem(s, 2)
        late = (s == 1) | (s == 5)
        g_load(s).wait()

        @pl.when(s == 0)
        def _():
            pltpu.make_async_copy(chunk_s.at[0], g_ref.at[rows(me)], loc.at[5]).start()

        @pl.when(jnp.logical_not(late) & (s > 0))
        def _():
            next_load(s + 1)

        d_out = _dot(chunk_s[slot], wo_s[...], 1, 1).astype(LOW)

        @pl.when(s == 0)
        def _():
            pltpu.make_async_copy(chunk_s.at[0], g_ref.at[rows(me)], loc.at[5]).wait()
            next_load(s + 1)

        deltas = []
        for h in range(heads):
            one = d_out[:, h * HEAD:(h + 1) * HEAD]
            do_s[h * tok:(h + 1) * tok, :] = one
            both = one.astype(F32) * seen_ref[rows(j), h * HEAD:(h + 1) * HEAD].astype(F32)
            top_s[:, strips[h]] = both.T.sum(axis=0, keepdims=True)
        dq_s[...] = jnp.zeros_like(dq_s)

        def block(i, masked):
            here = rows(i)
            scores = [_dot(k_s[here, :], q_s[j, at, :], 1, 1) for at in strips]
            dps = [_dot(v_s[here, :], do_s[at, :], 1, 1) for at in strips]
            for at, sc, dp in zip(strips, scores, dps):
                p = jnp.exp2(sc * e - lse_s[j, :, at])
                if masked:
                    p = jnp.where(visible(), p, 0.0)
                ds = (p * (dp - top_s[:, at])).astype(LOW)
                dv_s[here, :] += _dot(p.astype(LOW), do_s[at, :], 1, 0)
                dk_s[here, :] += _dot(ds, q_s[j, at, :], 1, 0)
                dq_s[:, at] += _dot(kt_s[:, here], ds, 1, 0)

        lax.fori_loop(0, j, lambda i, _: block(i, False), None)
        block(j, True)
        cos, sin = tables(j)
        for h in range(heads):
            one = (dq_s[:, strips[h]] * HEAD**-0.5).T.astype(LOW).astype(F32)
            grads_ref[rows(j), h * HEAD:(h + 1) * HEAD] = turned(one, cos, -sin)

        @pl.when(late)
        def _():
            next_load(s + 1)

    lax.fori_loop(0, n, backward, None)

    def finish(j, _):
        cos, sin = tables(j)
        at = rows(j)
        one = (dk_s[at, :] * HEAD**-0.5).astype(LOW).astype(F32)
        grads_ref[at, hw:hw + HEAD] = turned(one, cos, -sin)
        grads_ref[at, hw + HEAD:] = dv_s[at, :].astype(LOW)

    lax.fori_loop(0, n, finish, None)
    for z in range(2):
        for i in range(13):
            copy(z, i, sent[i]).wait_send()


def _back(n, heads, x_ref, dy_ref, gain_ref, grads_ref, seen_ref, wq_ref, wk_ref, wv_ref, a_ref, g_ref,
          dx_ref, by_gain_ref, by_wq_ref, by_wk_ref, by_wv_ref, by_wo_ref,
          w_s, turn_s, out_s, pair_s, ring_s, last_s, own_s, flow_s, dw_s, dwo_s, gain_s, send, recv, gsend, grecv, loc, sem_in, sem_out):
    tok, dim = dx_ref.shape
    half, hw = tok // 2, heads * HEAD
    width = hw + 2 * HEAD
    wide = dim // 4
    me, core, turn, right, left, across = _places(n)
    other = me + turn
    loads = [pltpu.make_async_copy(wq_ref, w_s.at[:, :hw], loc.at[0]),
             pltpu.make_async_copy(wk_ref, w_s.at[:, hw:hw + HEAD], loc.at[1]),
             pltpu.make_async_copy(wv_ref, w_s.at[:, hw + HEAD:], loc.at[2])]
    for load in loads:
        load.start()
    _greet([lax.rem(me + k, n) for k in range(1, n)])
    for load in loads:
        load.wait()

    def term(dst, dev, part, *adds):
        at = _at(dev * tok + part * half, half)

        def column(c, _):
            cols = _at(c * wide, wide)
            t = _dot(grads_ref[at, :], w_s[cols, :], 1, 1)
            for add in adds:
                t = t + add[:, cols].astype(F32)
            dst[:, cols] = t.astype(dst.dtype)

        lax.fori_loop(0, dim // wide, column, None)

    there = [across, right, left, me]
    plan = [(0, 0), (0, 1), (1, 1), (2, 0), (1, 0), (2, 1), (3, 0), (3, 1)]

    def copy(i, src, dst, dev):
        return pltpu.make_async_remote_copy(src_ref=src, dst_ref=dst, send_sem=send.at[i], recv_sem=recv.at[i], device_id={"tp": dev}, device_id_type=MESH)

    def pair(i):
        place, part = plan[i]
        return copy(i, out_s.at[i % 4], pair_s.at[place, part], other)

    ring = [copy(8, pair_s.at[0, 0], ring_s.at[0], right), copy(9, pair_s.at[1, 1], last_s.at[0, 1], right), copy(10, pair_s.at[1, 0], last_s.at[0, 0], right),
            copy(11, pair_s.at[0, 1], ring_s.at[1], left), copy(12, pair_s.at[2, 0], last_s.at[1, 0], left), copy(13, pair_s.at[2, 1], last_s.at[1, 1], left)]

    def give(i):
        place, part = plan[i]
        if i >= 4:
            pair(i - 4).wait_send()
        term(out_s.at[i % 4], there[place] + turn, part)
        pair(i).start()

    def take(i, *adds):
        place, part = plan[i]
        pair(i).wait_recv()
        slot = pair_s.at[place, part]
        term(slot, there[place], part, slot, *adds)

    give(0)
    give(1)
    take(0)
    ring[0].start()
    take(1)
    ring[3].start()
    give(2)
    give(3)
    take(2)
    ring[1].start()
    take(3)
    ring[4].start()
    for i in range(4, 8):
        give(i)

    def lay(j, _):
        at = _at(j * tok, tok)
        turn_s[:width, at] = grads_ref[at, :].T
        turn_s[width:, at] = seen_ref[at, :].T

    lax.fori_loop(0, n, lay, None)
    for i in (6, 7):
        part = plan[i][1]
        pair(i).wait_recv()
        term(own_s.at[pl.ds(part * half, half)], me, part, pair_s.at[3, part])

    block = dw_s.shape[1]
    blocks = dim // block

    def fetch(s, kind):
        src = (a_ref, g_ref)[kind]
        return pltpu.make_async_copy(src.at[:, _at(s * block, block)], flow_s.at[kind], sem_in.at[kind])

    def puts(s):
        at = _at(s * block, block)
        return [pltpu.make_async_copy(dw_s.at[0, :, :hw], by_wq_ref.at[at], sem_out.at[0]),
                pltpu.make_async_copy(dw_s.at[0, :, hw:hw + HEAD], by_wk_ref.at[at], sem_out.at[1]),
                pltpu.make_async_copy(dw_s.at[0, :, hw + HEAD:], by_wv_ref.at[at], sem_out.at[2])]

    def put_o(s):
        return pltpu.make_async_copy(dwo_s.at[0], by_wo_ref.at[:, _at(s * block, block)], sem_out.at[3])

    fetch(0, 0).start()
    fetch(0, 1).start()

    def weights(s, _):
        fetch(s, 0).wait()
        dw = _dot(turn_s[:width, :], flow_s[0], 1, 0)

        @pl.when(s + 1 < blocks)
        def _():
            fetch(s + 1, 0).start()

        @pl.when(s > 0)
        def _():
            for put in puts(s - 1):
                put.wait()

        dw_s[0] = dw.T.astype(LOW)
        for put in puts(s):
            put.start()
        fetch(s, 1).wait()
        dwo = _dot(turn_s[width:, :], flow_s[1], 1, 0)

        @pl.when(s + 1 < blocks)
        def _():
            fetch(s + 1, 1).start()

        @pl.when(s > 0)
        def _():
            put_o(s - 1).wait()

        dwo_s[0] = dwo.astype(LOW)
        put_o(s).start()

    lax.fori_loop(0, blocks // 2, weights, None)
    ring[0].wait_recv()
    take(4, ring_s.at[0])
    ring[2].start()
    ring[3].wait_recv()
    take(5, ring_s.at[1])
    ring[5].start()
    lax.fori_loop(blocks // 2, blocks, weights, None)
    for put in puts(blocks - 1):
        put.wait()
    put_o(blocks - 1).wait()

    xs = [pltpu.make_async_copy(x_ref.at[pl.ds(h * half, half)], pair_s.at[3, h], sem_in.at[h]) for h in range(2)]
    ds = [pltpu.make_async_copy(dy_ref.at[pl.ds(h * half, half)], ring_s.at[h], loc.at[h]) for h in range(2)]
    for load in xs + ds:
        load.start()
    for load in xs + ds:
        load.wait()
    for i in (1, 2, 4, 5):
        ring[i].wait_recv()
    gain = gain_ref[...].astype(F32)
    step = 32
    own_gain = gain_s.at[me]
    own_gain[...] = jnp.zeros((8, dim), F32)

    for h in range(2):
        def rows(r, _, h=h):
            at = _at(r * step, step)
            whole = _at(h * half + r * step, step)
            da = own_s[whole, :] + last_s[0, h, at, :].astype(F32) + last_s[1, h, at, :].astype(F32)
            da = da.astype(LOW).astype(F32)
            wide_x = pair_s[3, h, at, :].astype(F32)
            scale = lax.rsqrt(jnp.mean(wide_x * wide_x, -1, keepdims=True) + 1e-6)
            hat = wide_x * scale
            part = da * hat
            own_gain[...] += sum(part[k:k + 8] for k in range(0, step, 8))
            d_hat = da * gain
            inner = jnp.mean(d_hat * hat, -1, keepdims=True)
            dx = (d_hat - hat * inner) * scale
            dx_ref[whole, :] = (dx + ring_s[h, at, :].astype(F32)).astype(LOW)

        lax.fori_loop(0, half // step, rows, None)

    own_gain[0:1, :] = own_gain[...].sum(axis=0, keepdims=True)
    swaps = [pltpu.make_async_remote_copy(src_ref=gain_s.at[me, pl.ds(0, 1)], dst_ref=gain_s.at[me, pl.ds(0, 1)], send_sem=gsend.at[k - 1], recv_sem=grecv.at[k - 1],
                                          device_id={"tp": lax.rem(me + k, n)}, device_id_type=MESH) for k in range(1, n)]
    for swap in swaps:
        swap.start()
    for k in range(1, n):
        source = gain_s.at[lax.rem(me + n - k, n), pl.ds(0, 1)]
        pltpu.make_async_remote_copy(src_ref=source, dst_ref=source, send_sem=gsend.at[k - 1], recv_sem=grecv.at[k - 1],
                                     device_id={"tp": other}, device_id_type=MESH).wait_recv()
    by_gain_ref[...] = sum(gain_s[k, 0:1, :] for k in range(n))
    for swap in swaps:
        swap.wait_send()
    for i in range(4, 8):
        pair(i).wait_send()
    for one in ring:
        one.wait_send()


def solution(mesh):
    n = mesh.shape["tp"]

    def step(x, dy, gain, wq, wk, wv, wo):
        tok, dim = x.shape
        heads = wq.shape[1] // HEAD
        hw = heads * HEAD
        width = hw + 2 * HEAD
        rows, cols = n * tok, heads * tok
        freq = np.float64(THETA) ** (-np.arange(HEAD // 2) / (HEAD // 2))

        def table(places):
            angle = np.asarray(places, np.float64)[:, None] * freq
            cos, sin = np.cos(angle), np.sin(angle)
            return jnp.asarray(np.stack([np.concatenate([cos, cos], 1), np.concatenate([-sin, sin], 1)]), F32)

        near, far = table(np.arange(tok)), table(np.arange(n) * tok)
        gain = gain[None]
        anywhere, vmem = pl.BlockSpec(memory_space=pl.ANY), pl.BlockSpec(memory_space=pltpu.VMEM)
        dma, scratch = pltpu.SemaphoreType.DMA, pltpu.VMEM
        a, g, seen, grads = pl.pallas_call(
            functools.partial(_front, n, heads),
            out_shape=[jax.ShapeDtypeStruct((rows, dim), LOW)] * 2 + [jax.ShapeDtypeStruct((rows, hw), LOW), jax.ShapeDtypeStruct((rows, width), LOW)],
            in_specs=[anywhere, anywhere, vmem, anywhere, anywhere, anywhere, anywhere, vmem, vmem],
            out_specs=[anywhere, anywhere, vmem, vmem],
            scratch_shapes=[
                scratch((2, tok, dim), LOW), scratch((dim, width), LOW), scratch((hw, dim), LOW),
                scratch((n, cols, HEAD), LOW), scratch((rows, HEAD), LOW), scratch((HEAD, rows), LOW), scratch((rows, HEAD), LOW), scratch((HEAD + 8, rows), LOW),
                scratch((n, 1, cols), F32), scratch((cols, HEAD), LOW), scratch((1, cols), F32), scratch((HEAD + 8, cols), F32),
                scratch((HEAD, cols), F32), scratch((rows, HEAD), F32), scratch((rows, HEAD), F32),
                dma((2, 13)), dma((2, 13)), dma((6,))],
            compiler_params=pltpu.CompilerParams(collective_id=0, has_side_effects=True, vmem_limit_bytes=VMEM),
            name="front",
        )(x, dy, gain, wq, wk, wv, wo, near, far)
        block = HEAD * 3
        half = tok // 2
        dx, by_gain, by_wq, by_wk, by_wv, by_wo = pl.pallas_call(
            functools.partial(_back, n, heads),
            out_shape=[jax.ShapeDtypeStruct((tok, dim), LOW), jax.ShapeDtypeStruct((1, dim), F32), jax.ShapeDtypeStruct(wq.shape, LOW),
                       jax.ShapeDtypeStruct(wk.shape, LOW), jax.ShapeDtypeStruct(wv.shape, LOW), jax.ShapeDtypeStruct(wo.shape, LOW)],
            in_specs=[anywhere, anywhere, vmem, vmem, vmem, anywhere, anywhere, anywhere, anywhere, anywhere],
            out_specs=[vmem, vmem, anywhere, anywhere, anywhere, anywhere],
            scratch_shapes=[
                scratch((dim, width), LOW), scratch((width + hw, rows), LOW),
                scratch((4, half, dim), LOW), scratch((4, 2, half, dim), LOW), scratch((2, half, dim), LOW), scratch((2, 2, half, dim), LOW), scratch((tok, dim), F32),
                scratch((2, rows, block), LOW), scratch((1, block, width), LOW), scratch((1, hw, block), LOW), scratch((n, 8, dim), F32),
                dma((14,)), dma((14,)), dma((n - 1,)), dma((n - 1,)), dma((3,)), dma((2,)), dma((4,))],
            compiler_params=pltpu.CompilerParams(collective_id=1, has_side_effects=True, vmem_limit_bytes=VMEM),
            name="back",
        )(x, dy, gain, grads, seen, wq, wk, wv, a, g)
        return dx, by_gain, by_wq, by_wk, by_wv, by_wo

    tokens, columns = P(("dp", "tp"), None), P(None, "tp")
    return jax.shard_map(
        step,
        mesh=mesh,
        in_specs=(tokens, tokens, P(None), columns, columns, columns, P("tp", None)),
        out_specs=(tokens, P("dp", None), P("dp", "tp"), P("dp", "tp"), P("dp", "tp"), P(("dp", "tp"), None)),
        check_vma=False,
    )
```

```python
import functools

import jax
import jax.numpy as jnp
import numpy as np
from jax import lax
from jax.experimental import pallas as pl
from jax.experimental.pallas import tpu as pltpu
from jax.sharding import PartitionSpec as P

HEAD = 128
THETA = 10000
NEG = -1e30
HIDDEN = 2 * NEG
LOG2E = 1.4426950408889634
VMEM = 67_043_328
MESH = pl.DeviceIdType.MESH
F32, LOW = jnp.float32, jnp.bfloat16
PIECES = 16
SUBS = 3
LOADS = 4


def _dot(a, b, ca, cb):
    return lax.dot_general(a, b, (((ca,), (cb,)), ((), ())), preferred_element_type=F32)


def _at(start, size, unit=None):
    return pl.ds(pl.multiple_of(start, unit or size), size)


def _kernel(n, heads, x_ref, dy_ref, gain_ref, wq_ref, wk_ref, wv_ref, wo_ref, near_ref, far_ref,
            a_ref, g_ref, dx_ref, by_gain_ref, by_wq_ref, by_wk_ref, by_wv_ref, by_wo_ref,
            chunk_s, wt_s, wo_s, q_s, k_s, kt_s, v_s, vt_s, lse_s, do_s, delta_s, top_s, mix_s, dq_s, dk_s, dv_s, grads_s, turn_s,
            pair_s, ring_s, last_s, own_s, flow_s, dw_s, dwo_s, gain_s, sum_s, send, recv, rsend, rrecv, gsend, grecv, loc, sem_load, sem_in, sem_out):
    tok, dim = x_ref.shape
    half, quarter, hw = tok // 2, tok // 4, heads * HEAD
    width = hw + 2 * HEAD
    chips = n // 2
    me = lax.axis_index("tp")
    chip, core = me // 2, lax.rem(me, 2)
    other = chip * 2 + 1 - core
    lchip, rchip, ochip = lax.rem(chip + chips - 1, chips), lax.rem(chip + 1, chips), lax.rem(chip + chips // 2, chips)
    left, right, across = lchip * 2 + core, rchip * 2 + core, ochip * 2 + core
    e = HEAD**-0.5 * LOG2E

    def moved(c):
        return [(lchip, 0, half * c, half), (rchip, 0, half * c, half), (lchip, 1, half * c, half), (rchip, 1, half * c, half),
                (ochip, 0, half * c, half), (ochip, 1, half * c, half)]

    near_part, far_part = half * core, half * core + quarter
    sent = [(chip, 0, near_part, half), (chip, 1, near_part, half), (lchip, 0, near_part, quarter), (lchip, 1, near_part, quarter),
            (chip, 0, near_part, half), (chip, 1, near_part, half), (rchip, 0, far_part, quarter), (rchip, 1, far_part, quarter),
            (chip, core, half * (1 - core), half), *moved(core), (chip, core, near_part, half)]
    got = [(lchip, 0, near_part, half), (lchip, 1, near_part, half), (ochip, 0, near_part, quarter), (ochip, 1, near_part, quarter),
           (rchip, 0, near_part, half), (rchip, 1, near_part, half), (ochip, 0, far_part, quarter), (ochip, 1, far_part, quarter),
           (chip, 1 - core, near_part, half), *moved(1 - core), (chip, 1 - core, half * (1 - core), half)]
    to = [right] * 4 + [left] * 4 + [other] * 8

    def rows(dev):
        return _at(dev * tok, tok)

    def copy(z, i, what):
        c, k, first, size = what
        full = (a_ref, g_ref)[z].at[_at((c * 2 + k) * tok + first, size, quarter)]
        near = i in (8, 15)
        return pltpu.make_async_remote_copy(src_ref=chunk_s.at[z, _at(first, size, quarter)] if near else full, dst_ref=full, send_sem=send.at[z, i], recv_sem=recv.at[z, i],
                                            device_id={"tp": to[i]}, device_id_type=MESH)

    def start(z, *pieces):
        for i in pieces:
            copy(z, i, sent[i]).start()

    def arrived(z, *pieces):
        for i in pieces:
            copy(z, i, got[i]).wait_recv()

    def order(s):
        t = s // 2
        middle, final = (t + 1) // 2 - 2 * (t // 3), t // 3
        c = lax.rem(chip + middle * (chips - 1 - (chips - 2) * lax.rem(s, 2)) + final * (chips // 2), chips)
        k = (1 - middle - final) * lax.rem(core + s, 2) + middle * (t - 1) + final * lax.rem(s, 2)
        return c * 2 + k

    def pass_on(z, s):
        @pl.when(s == 2)
        def _():
            arrived(z, 0, 4)
            start(z, 2, 6, 9, 10)

        @pl.when(s == 4)
        def _():
            arrived(z, 1, 5)
            start(z, 3, 7, 11, 12)
            if z == 0:
                start(1, 0, 4, 1, 5)

        @pl.when(s == 6)
        def _():
            arrived(z, 2, 6)
            start(z, 13)

        @pl.when(s == 7)
        def _():
            arrived(z, 3, 7)
            start(z, 14)

    def load(z, s):
        dev, slot = order(s), lax.rem(s, 2)
        full = (a_ref, g_ref)[z]
        return [pltpu.make_async_copy(full.at[_at(dev * tok + k * (tok // LOADS), tok // LOADS)], chunk_s.at[slot, pl.ds(k * (tok // LOADS), tok // LOADS)], sem_load.at[slot, k])
                for k in range(LOADS)]

    def fetch_next(z, s):
        @pl.when(s == 2)
        def _():
            arrived(z, 9, 10)

        @pl.when(s == 4)
        def _():
            arrived(z, 11, 12)

        @pl.when(s == 6)
        def _():
            arrived(z, 13)

        @pl.when(s == 7)
        def _():
            arrived(z, 14)

        @pl.when(s < n)
        def _():
            for one in load(z, s):
                one.start()

    load_x = pltpu.make_async_copy(x_ref, chunk_s.at[0], loc.at[0])
    load_x.start()
    load_dy = pltpu.make_async_copy(dy_ref, chunk_s.at[1], loc.at[1])
    load_dy.start()
    loads = [pltpu.make_async_copy(wq_ref, q_s, loc.at[2]), pltpu.make_async_copy(wk_ref, k_s, loc.at[3]), pltpu.make_async_copy(wv_ref, v_s, loc.at[4])]
    for one in loads:
        one.start()
    load_wo = pltpu.make_async_copy(wo_ref, wo_s, loc.at[5])
    load_wo.start()
    barrier = pltpu.get_barrier_semaphore()
    for k in range(1, n):
        pl.semaphore_signal(barrier, inc=1, device_id={"tp": lax.rem(me + k, n)}, device_id_type=MESH)

    load_x.wait()
    gain = gain_ref[...].reshape(1, dim).astype(F32)
    block = 32

    def norm(r, _):
        at = _at(r * block, block)
        wide = chunk_s[0, at, :].astype(F32)
        scale = lax.rsqrt(jnp.mean(wide * wide, -1, keepdims=True) + 1e-6)
        chunk_s[0, at, :] = (wide * scale * gain).astype(LOW)

    lax.fori_loop(0, tok // block, norm, None)
    pl.semaphore_wait(barrier, n - 1)
    start(0, 8, 15)
    keep = pltpu.make_async_copy(chunk_s.at[0], a_ref.at[rows(me)], loc.at[0])
    keep.start()
    load_dy.wait()
    keep_dy = pltpu.make_async_copy(chunk_s.at[1], g_ref.at[rows(me)], loc.at[1])
    keep_dy.start()
    keep.wait()
    arrived(0, 8)
    start(0, 0, 4, 1, 5)
    start(1, 8, 15)
    keep_dy.wait()
    for one in loads:
        one.wait()

    def lay_weights(i, _):
        at = _at(i * tok, tok)
        wt_s[:hw, at] = q_s[at, :].T
        wt_s[hw:hw + HEAD, at] = k_s[at, :].T
        wt_s[hw + HEAD:, at] = v_s[at, :].T

    lax.fori_loop(0, dim // tok, lay_weights, None)
    arrived(0, 15)
    arrived(1, 8, 15)
    for z in range(2):
        for i in (8, 15):
            copy(z, i, sent[i]).wait_send()

    cols = heads * tok
    strips = [pl.ds(h * tok, tok) for h in range(heads)]
    lanes = [pl.ds(h * HEAD, HEAD) for h in range(heads)]

    def tables(j):
        ca, sa = near_ref[0], near_ref[1]
        cb, sb = far_ref[0, pl.ds(j, 1), :], far_ref[1, pl.ds(j, 1), :]
        return ca * cb - sa * sb, sa * cb + ca * sb

    def turned(t, cos, sin):
        return (t * cos + pltpu.roll(t, HEAD // 2, 1) * sin).astype(LOW)

    def project(j, slot):
        y = _dot(chunk_s[slot], wt_s[...], 1, 1).astype(LOW).astype(F32)
        cos, sin = tables(j)
        at = rows(j)
        for h in range(heads):
            q_s[at, lanes[h]] = turned(y[:, h * HEAD:(h + 1) * HEAD], cos, sin)
        k = turned(y[:, hw:hw + HEAD], cos, sin)
        v = y[:, hw + HEAD:].astype(LOW)
        k_s[at, :] = k
        kt_s[:, at] = k.T
        v_s[at, :] = v
        vt_s[:HEAD, at] = v.T

    def visible():
        return lax.broadcasted_iota(jnp.int32, (tok, tok), 1) >= lax.broadcasted_iota(jnp.int32, (tok, tok), 0)

    def seen_block(j, i, masked):
        here = rows(i)
        scores = [_dot(k_s[here, :], q_s[rows(j), at], 1, 1) for at in lanes]
        weights, keeps = [], []
        for at, s in zip(strips, scores):
            if masked:
                s = jnp.where(visible(), s, HIDDEN)
            old = top_s[j, :, at]
            top = jnp.maximum(old, s.max(axis=0, keepdims=True))
            top_s[j, :, at] = top
            weights.append(jnp.exp2((s - top) * e).astype(LOW))
            keeps.append(jnp.exp2((old - top) * e))
        for at, p, kept in zip(strips, weights, keeps):
            mix_s[j, :, at] = mix_s[j, :, at] * kept + _dot(vt_s[:, here], p, 1, 0)

    vt_s[HEAD:, :] = jnp.ones((8, n * tok), LOW)

    def clear(j, _):
        top_s[j] = jnp.full((1, cols), NEG, F32)
        mix_s[j] = jnp.zeros((HEAD + 8, cols), F32)

    lax.fori_loop(0, n, clear, None)
    dk_s[...] = jnp.zeros_like(dk_s)
    dv_s[...] = jnp.zeros_like(dv_s)

    def x_step(s, _):
        j = order(s)
        early = (lax.rem(s, 2) == 0) & (s < 6)
        middle = (s == 5) | (s == 6)

        @pl.when(s > 0)
        def _():
            for one in load(0, s):
                one.wait()

        @pl.when(early)
        def _():
            fetch_next(0, s + 1)

        project(j, lax.rem(s, 2))

        @pl.when(middle)
        def _():
            pass_on(0, s + 1)

        seen_block(j, j, True)

        @pl.when(middle)
        def _():
            fetch_next(0, s + 1)

        def earlier(t, _):
            i = order(t)
            seen_block(jnp.maximum(i, j), jnp.minimum(i, j), False)

        lax.fori_loop(0, s, earlier, None)

        @pl.when((s == 1) | (s == 3))
        def _():
            pass_on(0, s + 1)
            fetch_next(0, s + 1)

    lax.fori_loop(0, n, x_step, None)

    load_wo.wait()

    for one in load(1, 0):
        one.start()

    def backward(s, _):
        j = order(s)
        slot = lax.rem(s, 2)
        early = (lax.rem(s, 2) == 0) & (s < 6)
        for one in load(1, s):
            one.wait()

        @pl.when(early)
        def _():
            fetch_next(1, s + 1)

        d_out = _dot(chunk_s[slot], wo_s[...], 1, 1).astype(LOW)
        total = mix_s[j, HEAD:HEAD + 1, :]
        lse_s[...] = top_s[j] * e + jnp.log2(total)
        for h in range(heads):
            out = (mix_s[j, :HEAD, strips[h]] * (1 / total[:, h * tok:(h + 1) * tok])).astype(LOW)
            turn_s[pl.ds(width + h * HEAD, HEAD), rows(j)] = out
            one = d_out[:, h * HEAD:(h + 1) * HEAD]
            do_s[:, lanes[h]] = one
            delta_s[:, strips[h]] = (one.astype(F32).T * out.astype(F32)).sum(axis=0, keepdims=True)
        dq_s[...] = jnp.zeros_like(dq_s)

        def block(i, masked):
            here = rows(i)
            scores = [_dot(k_s[here, :], q_s[rows(j), at], 1, 1) for at in lanes]
            dps = [_dot(v_s[here, :], do_s[:, at], 1, 1) for at in lanes]
            for at, lane, sc, dp in zip(strips, lanes, scores, dps):
                p = jnp.exp2(sc * e - lse_s[:, at])
                if masked:
                    p = jnp.where(visible(), p, 0.0)
                ds = (p * (dp - delta_s[:, at])).astype(LOW)
                dv_s[here, :] += _dot(p.astype(LOW), do_s[:, lane], 1, 0)
                dk_s[here, :] += _dot(ds, q_s[rows(j), lane], 1, 0)
                dq_s[:, at] += _dot(kt_s[:, here], ds, 1, 0)

        lead = jnp.maximum(j - 2, 0)

        def whole(i, _):
            @pl.when(jnp.logical_not(early) & (i == lead))
            def _():
                pass_on(1, s + 1)

            block(i, False)

        lax.fori_loop(0, j, whole, None)

        @pl.when(jnp.logical_not(early))
        def _():
            @pl.when(j == 0)
            def _():
                pass_on(1, s + 1)

            fetch_next(1, s + 1)

        block(j, True)
        cos, sin = tables(j)
        for h in range(heads):
            one = (dq_s[:, strips[h]] * HEAD**-0.5).T.astype(LOW).astype(F32)
            grads_s[rows(j), lanes[h]] = turned(one, cos, -sin)

    lax.fori_loop(0, n, backward, None)

    def finish(j, _):
        cos, sin = tables(j)
        at = rows(j)
        one = (dk_s[at, :] * HEAD**-0.5).astype(LOW).astype(F32)
        grads_s[at, hw:hw + HEAD] = turned(one, cos, -sin)
        grads_s[at, hw + HEAD:] = dv_s[at, :].astype(LOW)

    lax.fori_loop(0, n, finish, None)

    wide = dim // 2

    def term(dst, dev, part, *adds):
        at = _at(dev * tok + part * half, half)

        def column(c, _):
            here = _at(c * wide, wide)
            t = _dot(grads_s[at, :], wt_s[:, here], 1, 0)
            for add in adds:
                t = t + add[:, here].astype(F32)
            dst[:, here] = t.astype(dst.dtype)

        lax.fori_loop(0, dim // wide, column, None)

    there = [ochip, rchip, lchip, chip]
    plan = [(0, 0), (0, 1), (1, 1), (2, 0), (1, 0), (2, 1), (3, 0), (3, 1)]

    def remote(i, src, dst, dev):
        return pltpu.make_async_remote_copy(src_ref=src, dst_ref=dst, send_sem=rsend.at[i], recv_sem=rrecv.at[i], device_id={"tp": dev}, device_id_type=MESH)

    def out(i):
        return chunk_s.at[i % 4 // 2, pl.ds(i % 2 * half, half)]

    def pair(i):
        place, part = plan[i]
        return remote(i, out(i), pair_s.at[place, part], other)

    sub = half // SUBS
    parts = [pl.ds(k * sub, sub) for k in range(SUBS)]
    ring_a = [remote(8, pair_s.at[0, 0], ring_s.at[0], right), remote(9, pair_s.at[0, 1], ring_s.at[1], left)]
    ring_b = [remote(10, pair_s.at[1, 1], last_s.at[0, 1], right), remote(11, pair_s.at[2, 0], last_s.at[1, 0], left)]
    ring_c = [[remote(12 + k, pair_s.at[1, 0, p], last_s.at[0, 0, p], right) for k, p in enumerate(parts)],
              [remote(12 + SUBS + k, pair_s.at[2, 1, p], last_s.at[1, 1, p], left) for k, p in enumerate(parts)]]

    def give(i):
        place, part = plan[i]
        if i >= 4:
            pair(i - 4).wait_send()
        term(out(i), there[place] * 2 + 1 - core, part)
        pair(i).start()

    def take(i, *adds):
        place, part = plan[i]
        pair(i).wait_recv()
        slot = pair_s.at[place, part]
        term(slot, there[place] * 2 + core, part, slot, *adds)

    give(0)
    give(1)
    take(0)
    ring_a[0].start()
    take(1)
    ring_a[1].start()
    give(2)
    give(3)
    take(2)
    ring_b[0].start()
    take(3)
    ring_b[1].start()
    for i in range(4, 8):
        give(i)

    def lay(j, _):
        turn_s[:width, rows(j)] = grads_s[rows(j), :].T

    lax.fori_loop(0, n, lay, None)
    for i in (6, 7):
        part = plan[i][1]
        pair(i).wait_recv()
        term(own_s.at[pl.ds(part * half, half)], me, part, pair_s.at[3, part])

    size = dw_s.shape[0]
    blocks = dim // size
    flows = [q_s, flow_s]

    def fetch(s, kind):
        return pltpu.make_async_copy((a_ref, g_ref)[kind].at[:, _at(s * size, size)], flows[kind], sem_in.at[kind])

    def puts(s):
        at = _at(s * size, size)
        return [pltpu.make_async_copy(dw_s.at[:, :hw], by_wq_ref.at[at], sem_out.at[0]),
                pltpu.make_async_copy(dw_s.at[:, hw:hw + HEAD], by_wk_ref.at[at], sem_out.at[1]),
                pltpu.make_async_copy(dw_s.at[:, hw + HEAD:], by_wv_ref.at[at], sem_out.at[2])]

    def put_o(s):
        return pltpu.make_async_copy(dwo_s, by_wo_ref.at[:, _at(s * size, size)], sem_out.at[3])

    fetch(0, 0).start()
    fetch(0, 1).start()

    def weights(s, _):
        fetch(s, 0).wait()
        dw = _dot(turn_s[:width, :], flows[0][...], 1, 0)

        @pl.when(s + 1 < blocks)
        def _():
            fetch(s + 1, 0).start()

        @pl.when(s > 0)
        def _():
            for put in puts(s - 1):
                put.wait()

        dw_s[...] = dw.T.astype(LOW)
        for put in puts(s):
            put.start()
        fetch(s, 1).wait()
        dwo = _dot(turn_s[width:, :], flows[1][...], 1, 0)

        @pl.when(s + 1 < blocks)
        def _():
            fetch(s + 1, 1).start()

        @pl.when(s > 0)
        def _():
            put_o(s - 1).wait()

        dwo_s[...] = dwo.astype(LOW)
        put_o(s).start()

    lax.fori_loop(0, blocks // 2, weights, None)
    ring_a[0].wait_recv()
    take(4, ring_s.at[0])
    for one in ring_c[0]:
        one.start()
    ring_a[1].wait_recv()
    take(5, ring_s.at[1])
    for one in ring_c[1]:
        one.start()
    lax.fori_loop(blocks // 2, blocks, weights, None)
    for put in puts(blocks - 1):
        put.wait()
    put_o(blocks - 1).wait()

    pulls = [pltpu.make_async_copy(x_ref.at[pl.ds(h * half, half)], pair_s.at[3, h], loc.at[h]) for h in range(2)]
    pulls += [pltpu.make_async_copy(dy_ref.at[pl.ds(h * half, half)], ring_s.at[h], loc.at[2 + h]) for h in range(2)]
    for pull in pulls:
        pull.start()
    sum_s[...] = jnp.zeros_like(sum_s)
    for pull in pulls:
        pull.wait()
    for one in ring_b:
        one.wait_recv()
    step = 32

    def normal(h, at):
        wide_x = pair_s[3, h, at, :].astype(F32)
        scale = lax.rsqrt(jnp.mean(wide_x * wide_x, -1, keepdims=True) + 1e-6)
        return wide_x * scale, scale

    def total_rows(k, h):
        def some(r, _):
            at = _at(k * sub + r * step, step)
            whole = _at(h * half + k * sub + r * step, step)
            da = (own_s[whole, :] + last_s[0, h, at, :].astype(F32) + last_s[1, h, at, :].astype(F32)).astype(LOW)
            last_s[0, h, at, :] = da
            both = da.astype(F32) * normal(h, at)[0]
            sum_s[...] += sum(both[i:i + 8] for i in range(0, step, 8))

        lax.fori_loop(0, sub // step, some, None)

    def x_rows(k, h):
        def some(r, _):
            at = _at(k * sub + r * step, step)
            hat, scale = normal(h, at)
            d_hat = last_s[0, h, at, :].astype(F32) * gain
            inner = jnp.mean(d_hat * hat, -1, keepdims=True)
            ring_s[h, at, :] = ((d_hat - hat * inner) * scale + ring_s[h, at, :].astype(F32)).astype(LOW)

        lax.fori_loop(0, sub // step, some, None)
        save = pltpu.make_async_copy(ring_s.at[h, parts[k]], dx_ref.at[pl.ds(h * half + k * sub, sub)], sem_out.at[4 + 2 * k + h])
        save.start()
        return save

    def swap(k, dev, owner):
        line = gain_s.at[owner]
        return pltpu.make_async_remote_copy(src_ref=line, dst_ref=line, send_sem=gsend.at[k - 1], recv_sem=grecv.at[k - 1], device_id={"tp": dev}, device_id_type=MESH)

    saves = []
    for k in range(SUBS):
        for h in range(2):
            ring_c[h][k].wait_recv()
            total_rows(k, h)
        if k == SUBS - 1:
            gain_s[me] = sum_s[...].sum(axis=0, keepdims=True)
            for i in range(1, n):
                swap(i, lax.rem(me + i, n), me).start()
        saves += [x_rows(k, h) for h in range(2)]
    for k in range(1, n):
        swap(k, other, lax.rem(me + n - k, n)).wait_recv()
    by_gain_ref[...] = sum(gain_s[k] for k in range(n))
    for k in range(1, n):
        swap(k, lax.rem(me + k, n), me).wait_send()
    for z in range(2):
        for i in range(PIECES):
            if i not in (8, 15):
                copy(z, i, sent[i]).wait_send()
    for i in range(4, 8):
        pair(i).wait_send()
    for one in [*ring_a, *ring_b, *ring_c[0], *ring_c[1]]:
        one.wait_send()
    for save in saves:
        save.wait()


def _results(*refs):
    k = len(refs) // 3
    sources, targets, rooms = refs[:k], refs[k:2 * k], refs[2 * k:3 * k]
    into, out = refs[-2:]
    pulls = [pltpu.make_async_copy(a, b, into.at[i]) for i, (a, b) in enumerate(zip(sources, rooms))]
    puts = [pltpu.make_async_copy(a, b, out.at[i]) for i, (a, b) in enumerate(zip(rooms, targets))]
    for pull in pulls:
        pull.start()
    for pull, put in zip(pulls, puts):
        pull.wait()
        put.start()
    for put in puts:
        put.wait()


def solution(mesh):
    n = mesh.shape["tp"]

    def step(x, dy, gain, wq, wk, wv, wo):
        tok, dim = x.shape
        heads = wq.shape[1] // HEAD
        hw = heads * HEAD
        width = hw + 2 * HEAD
        rows, cols, half = n * tok, heads * tok, tok // 2
        freq = np.float64(THETA) ** (-np.arange(HEAD // 2) / (HEAD // 2))

        def table(places):
            angle = np.asarray(places, np.float64)[:, None] * freq
            cos, sin = np.cos(angle), np.sin(angle)
            return jnp.asarray(np.stack([np.concatenate([cos, cos], 1), np.concatenate([-sin, sin], 1)]), F32)

        near, far = table(np.arange(tok)), table(np.arange(n) * tok)
        anywhere, vmem = pl.BlockSpec(memory_space=pl.ANY), pl.BlockSpec(memory_space=pltpu.VMEM)
        dma, scratch, shape = pltpu.SemaphoreType.DMA, pltpu.VMEM, jax.ShapeDtypeStruct
        size = hw
        most = max(rows, dim)
        ring = 12 + 2 * SUBS
        _, _, *results = pl.pallas_call(
            functools.partial(_kernel, n, heads),
            out_shape=[shape((rows, dim), LOW), shape((rows, dim), LOW), shape((tok, dim), LOW), shape((1, dim), F32),
                       shape(wq.shape, LOW), shape(wk.shape, LOW), shape(wv.shape, LOW), shape(wo.shape, LOW)],
            in_specs=[anywhere, anywhere, vmem, anywhere, anywhere, anywhere, anywhere, vmem, vmem],
            out_specs=[anywhere, anywhere, anywhere, vmem, anywhere, anywhere, anywhere, anywhere],
            scratch_shapes=[
                scratch((2, tok, dim), LOW), scratch((width, dim), LOW), scratch((hw, dim), LOW),
                scratch((most, hw), LOW), scratch((most, HEAD), LOW), scratch((HEAD, rows), LOW), scratch((most, HEAD), LOW), scratch((HEAD + 8, rows), LOW),
                scratch((1, cols), F32), scratch((tok, hw), LOW), scratch((1, cols), F32), scratch((n, 1, cols), F32), scratch((n, HEAD + 8, cols), F32),
                scratch((HEAD, cols), F32), scratch((rows, HEAD), F32), scratch((rows, HEAD), F32), scratch((rows, width), LOW), scratch((width + hw, rows), LOW),
                scratch((4, 2, half, dim), LOW), scratch((2, half, dim), LOW), scratch((2, 2, half, dim), LOW), scratch((tok, dim), F32),
                scratch((most, size), LOW), scratch((size, width), LOW), scratch((hw, size), LOW), scratch((n, 1, dim), F32), scratch((8, dim), F32),
                dma((2, PIECES)), dma((2, PIECES)), dma((ring,)), dma((ring,)), dma((n - 1,)), dma((n - 1,)), dma((6,)), dma((2, LOADS)), dma((2,)), dma((4 + 2 * SUBS,))],
            compiler_params=pltpu.CompilerParams(collective_id=0, has_side_effects=True, vmem_limit_bytes=VMEM),
            name="layer",
        )(x, dy, gain, wq, wk, wv, wo, near, far)
        kept = [results[i] for i in (2, 3, 4, 0, 5, 1)]
        out = pl.pallas_call(
            _results,
            out_shape=[shape(t.shape, t.dtype) for t in kept],
            in_specs=[anywhere] * len(kept),
            out_specs=[anywhere] * len(kept),
            scratch_shapes=[*[scratch(t.shape, t.dtype) for t in kept], dma((len(kept),)), dma((len(kept),))],
            compiler_params=pltpu.CompilerParams(vmem_limit_bytes=VMEM),
            name="results",
        )(*kept)
        return out[3], out[5], out[0], out[1], out[2], out[4]

    tokens, columns = P(("dp", "tp"), None), P(None, "tp")
    return jax.shard_map(
        step,
        mesh=mesh,
        in_specs=(tokens, tokens, P(None), columns, columns, columns, P("tp", None)),
        out_specs=(tokens, P("dp", None), P("dp", "tp"), P("dp", "tp"), P("dp", "tp"), P(("dp", "tp"), None)),
        check_vma=False,
    )
```

```python
import functools

import jax
import jax.numpy as jnp
import numpy as np
from jax import lax
from jax.experimental import pallas as pl
from jax.experimental.pallas import tpu as pltpu
from jax.sharding import PartitionSpec as P

HEAD = 128
THETA = 10000
NEG = -1e30
HIDDEN = 2 * NEG
LOG2E = 1.4426950408889634
VMEM = 67_043_328
MESH = pl.DeviceIdType.MESH
F32, LOW = jnp.float32, jnp.bfloat16
UNITS = 3
SUBS = 3


def _dot(a, b, ca, cb):
    return lax.dot_general(a, b, (((ca,), (cb,)), ((), ())), preferred_element_type=F32)


def _at(start, size, unit=None):
    return pl.ds(pl.multiple_of(start, unit or size), size)


def _kernel(n, heads, x_ref, dy_ref, gain_ref, wq_ref, wk_ref, wv_ref, wo_ref, near_ref, far_ref,
            a_ref, g_ref, dx_ref, by_gain_ref, by_wq_ref, by_wk_ref, by_wv_ref, by_wo_ref,
            chunk_s, wt_s, wo_s, q_s, k_s, kt_s, v_s, vt_s, lse_s, do_s, do_u, q_u, delta_s, top_s, mix_s, dq_s, dk_s, dv_s, grads_s, turn_s,
            pair_s, ring_s, last_s, own_s, flow_s, dw_s, dwo_s, gain_s, sum_s, send, recv, rsend, rrecv, gsend, grecv, loc, sem_wo, sem_load, sem_in, sem_out):
    tok, dim = x_ref.shape
    half, quarter, hw = tok // 2, tok // 4, heads * HEAD
    unit = tok // UNITS
    width = hw + 2 * HEAD
    chips = n // 2
    me = lax.axis_index("tp")
    chip, core = me // 2, lax.rem(me, 2)
    other = chip * 2 + 1 - core
    lchip, rchip, ochip = lax.rem(chip + chips - 1, chips), lax.rem(chip + 1, chips), lax.rem(chip + chips // 2, chips)
    left, right, across = lchip * 2 + core, rchip * 2 + core, ochip * 2 + core
    e = HEAD**-0.5 * LOG2E

    few = unit // 4

    def part(c):
        return unit // 2 * c

    away = 1 - core
    pieces = {}

    def piece(name, sent, got, to, size=2 * few):
        pieces[name] = (len(pieces) * UNITS, sent, got, to, size)

    for name, to, c_from in (("r", right, lchip), ("l", left, rchip)):
        for k in range(2):
            piece(name + str(k), (chip, k, part(core)), (c_from, k, part(core)), to)
    piece("p", (chip, core, part(away)), (chip, away, part(core)), other)
    piece("q", (chip, core, part(core)), (chip, away, part(away)), other)
    for name, c in (("pl", lchip), ("pr", rchip), ("po", ochip)):
        for k in range(2):
            piece(name + str(k), (c, k, part(core)), (c, k, part(away)), other)
    full_pieces = len(pieces)
    for name, to, c_over, shift in (("r", right, lchip, 0), ("l", left, rchip, few)):
        for k in range(2):
            piece(name + str(k + 2), (c_over, k, part(core) + shift), (ochip, k, part(core) + shift), to, few)

    def each(do):
        lax.fori_loop(0, UNITS, lambda k, _: do(k), None)

    def rows(dev):
        return _at(dev * tok, tok)

    def copy(z, name, k, sending=True):
        i, sent, got, to, size = pieces[name]
        c, e_, first = sent if sending else got
        at = first + unit * k
        full = (a_ref, g_ref)[z].at[_at((c * 2 + e_) * tok + at, size, few)]
        own = name in ("p", "q")
        return pltpu.make_async_remote_copy(src_ref=chunk_s.at[z, _at(at, size, few)] if own else full, dst_ref=full,
                                            send_sem=send.at[z, i + k], recv_sem=recv.at[z, i + k], device_id={"tp": to}, device_id_type=MESH)

    def start(z, k, *names):
        for name in names:
            copy(z, name, k).start()

    def arrived(z, k, *names):
        for name in names:
            copy(z, name, k, False).wait_recv()

    def order(s):
        t = s // 2
        middle, final = (t + 1) // 2 - 2 * (t // 3), t // 3
        c = lax.rem(chip + middle * (chips - 1 - (chips - 2) * lax.rem(s, 2)) + final * (chips // 2), chips)
        k = (1 - middle - final) * lax.rem(core + s, 2) + middle * (t - 1) + final * lax.rem(s, 2)
        return c * 2 + k

    def load(z, s, k):
        dev, slot = order(s), lax.rem(s, 2)
        return pltpu.make_async_copy((a_ref, g_ref)[z].at[_at(dev * tok + k * unit, unit)], chunk_s.at[slot, _at(k * unit, unit)], sem_load.at[slot, k])

    def pass_on(z, s):
        for e_ in range(2):

            @pl.when(s == 2 + 2 * e_)
            def _(e_=str(e_), over=str(e_ + 2)):
                def one(k):
                    arrived(z, k, "r" + e_, "l" + e_)
                    start(z, k, "r" + over, "l" + over, "pl" + e_, "pr" + e_)

                def rest(k):
                    arrived(z, k, "pl" + e_)
                    load(z, s, k).start()

                def both(k):
                    one(k)
                    rest(k)

                if z == 1:
                    each(one)
                    return

                lax.fori_loop(0, UNITS - 1, lambda k, _: both(k), None)
                one(UNITS - 1)
                if z == 0 and e_ == "1":
                    each(lambda k: start(1, k, "r0", "l0"))
                    each(lambda k: start(1, k, "r1", "l1"))
                rest(UNITS - 1)

            @pl.when(s == 6 + e_)
            def _(e_=str(e_), over=str(e_ + 2)):
                def one(k):
                    arrived(z, k, "r" + over, "l" + over)
                    start(z, k, "po" + e_)

                each(one)

    def fetch_next(z, s):
        for step, name in ((3, "pr0"), (5, "pr1"), (6, "po0"), (7, "po1")):

            @pl.when(s == step)
            def _(name=name):
                each(lambda k: arrived(z, k, name))

        if z == 1:

            @pl.when(s == 2)
            def _():
                each(lambda k: arrived(z, k, "pl0"))

            @pl.when(s == 4)
            def _():
                each(lambda k: arrived(z, k, "pl1"))

            each(lambda k: load(z, s, k).start())
            return

        @pl.when((s < n) & (s != 2) & (s != 4))
        def _():
            each(lambda k: load(z, s, k).start())

    load_x = pltpu.make_async_copy(x_ref, chunk_s.at[0], loc.at[0])
    load_x.start()
    load_dy = pltpu.make_async_copy(dy_ref, chunk_s.at[1], loc.at[1])
    load_dy.start()
    loads = [pltpu.make_async_copy(wq_ref, flow_s, loc.at[2]), pltpu.make_async_copy(wk_ref, k_s, loc.at[3]), pltpu.make_async_copy(wv_ref, v_s, loc.at[4])]
    for one in loads:
        one.start()
    loads += [pltpu.make_async_copy(wo_ref.at[:, pl.ds(i * hw, hw)], wo_s.at[pl.ds(i * hw, hw)], sem_wo.at[i]) for i in range(dim // hw)]
    for one in loads[3:]:
        one.start()
    barrier = pltpu.get_barrier_semaphore()
    for k in range(1, n):
        pl.semaphore_signal(barrier, inc=1, device_id={"tp": lax.rem(me + k, n)}, device_id_type=MESH)

    load_x.wait()
    gain = gain_ref[...].reshape(1, dim).astype(F32)
    block = 32

    def norm(r, _):
        at = _at(r * block, block)
        wide = chunk_s[0, at, :].astype(F32)
        scale = lax.rsqrt(jnp.mean(wide * wide, -1, keepdims=True) + 1e-6)
        chunk_s[0, at, :] = (wide * scale * gain).astype(LOW)

    lax.fori_loop(0, tok // block, norm, None)
    pl.semaphore_wait(barrier, n - 1)
    each(lambda k: start(0, k, "p"))
    each(lambda k: start(0, k, "q"))
    keep = pltpu.make_async_copy(chunk_s.at[0], a_ref.at[rows(me)], loc.at[0])
    keep.start()
    load_dy.wait()
    keep_dy = pltpu.make_async_copy(chunk_s.at[1], g_ref.at[rows(me)], loc.at[1])
    keep_dy.start()
    keep.wait()
    each(lambda k: arrived(0, k, "p"))
    each(lambda k: start(0, k, "r0", "l0"))
    each(lambda k: start(0, k, "r1", "l1"))
    each(lambda k: start(1, k, "p", "q"))
    keep_dy.wait()
    for one in loads:
        one.wait()

    def lay_weights(i, _):
        at = _at(i * tok, tok)
        wt_s[:hw, at] = flow_s[at, :].T
        wt_s[hw:hw + HEAD, at] = k_s[at, :].T
        wt_s[hw + HEAD:, at] = v_s[at, :].T

    def lay_wo(i, _):
        at = _at(i * hw, hw)
        wo_s[at, :] = wo_s[at, :].T

    lax.fori_loop(0, dim // tok, lay_weights, None)
    lax.fori_loop(0, dim // hw, lay_wo, None)
    each(lambda k: arrived(0, k, "q"))
    each(lambda k: arrived(1, k, "p", "q"))
    for z in range(2):
        each(lambda k, z=z: [copy(z, name, k).wait_send() for name in ("p", "q")] and None)

    cols = heads * tok
    strips = [pl.ds(h * tok, tok) for h in range(heads)]
    lanes = [pl.ds(h * HEAD, HEAD) for h in range(heads)]

    def tables(j, at=slice(None)):
        ca, sa = near_ref[0, at, :], near_ref[1, at, :]
        cb, sb = far_ref[0, pl.ds(j, 1), :], far_ref[1, pl.ds(j, 1), :]
        return ca * cb - sa * sb, sa * cb + ca * sb

    def turned(t, cos, sin):
        return (t * cos + pltpu.roll(t, HEAD // 2, 1) * sin).astype(LOW)

    def project(j, slot):
        y = _dot(chunk_s[slot], wt_s[...], 1, 1).astype(LOW).astype(F32)
        cos, sin = tables(j)
        at = rows(j)
        for h in range(heads):
            q_s[j, strips[h], :] = turned(y[:, h * HEAD:(h + 1) * HEAD], cos, sin)
        k = turned(y[:, hw:hw + HEAD], cos, sin)
        v = y[:, hw + HEAD:].astype(LOW)
        k_s[at, :] = k
        kt_s[:, at] = k.T
        v_s[at, :] = v
        vt_s[:HEAD, at] = v.T

    def visible():
        return lax.broadcasted_iota(jnp.int32, (tok, tok), 1) >= lax.broadcasted_iota(jnp.int32, (tok, tok), 0)

    def seen_block(j, i, masked):
        here = rows(i)
        wide = _dot(k_s[here, :], q_s[j], 1, 1)
        scores = [wide[:, h * tok:(h + 1) * tok] for h in range(heads)]
        weights, keeps = [], []
        for at, s in zip(strips, scores):
            if masked:
                s = jnp.where(visible(), s, HIDDEN)
            old = top_s[j, :, at]
            top = jnp.maximum(old, s.max(axis=0, keepdims=True))
            top_s[j, :, at] = top
            weights.append(jnp.exp2((s - top) * e).astype(LOW))
            keeps.append(jnp.exp2((old - top) * e))
        for at, p, kept in zip(strips, weights, keeps):
            mix_s[j, :, at] = mix_s[j, :, at] * kept + _dot(vt_s[:, here], p, 1, 0)

    vt_s[HEAD:, :] = jnp.ones((8, n * tok), LOW)

    def clear(j, _):
        top_s[j] = jnp.full((1, cols), NEG, F32)
        mix_s[j] = jnp.zeros((HEAD + 8, cols), F32)

    lax.fori_loop(0, n, clear, None)
    dk_s[...] = jnp.zeros_like(dk_s)
    dv_s[...] = jnp.zeros_like(dv_s)

    def keep_d_out(slot):
        d_out = _dot(chunk_s[slot], wo_s[...], 1, 0).astype(LOW)
        for h in range(heads):
            do_s[slot, strips[h], :] = d_out[:, h * HEAD:(h + 1) * HEAD]

    def x_step(s, _):
        j = order(s)
        early = (lax.rem(s, 2) == 0) & (s < 6)
        middle = (s == 5) | (s == 6)

        @pl.when(s > 0)
        def _():
            each(lambda k: load(0, s, k).wait())

        @pl.when(early)
        def _():
            fetch_next(0, s + 1)

        project(j, lax.rem(s, 2))

        seen_block(j, j, True)

        def earlier(t, _):
            @pl.when(middle & (t == 2 * (s - 5)))
            def _():
                pass_on(0, s + 1)

            @pl.when(middle & (t == 2 * (s - 4)))
            def _():
                fetch_next(0, s + 1)

            i = order(t)
            seen_block(jnp.maximum(i, j), jnp.minimum(i, j), False)

        lax.fori_loop(0, s, earlier, None)

        @pl.when(s == 1)
        def _():
            for t in range(2):
                each(lambda k, t=t: load(1, t, k).start())

            def one(t, _):
                each(lambda k: load(1, t, k).wait())
                keep_d_out(t)

            lax.fori_loop(0, 2, one, None)

        @pl.when((s == 1) | (s == 3))
        def _():
            pass_on(0, s + 1)
            fetch_next(0, s + 1)

    lax.fori_loop(0, n, x_step, None)


    steps = 4 * UNITS
    wraps = rchip > ochip
    turns = ochip == chips - 1
    pause = jnp.where(turns, steps, steps - UNITS)

    def unit_order(t):
        g = t // UNITS
        first = turns & (g < 2)
        side = jnp.where(first, lax.rem(t, 2), jnp.where(turns, 2, jnp.where(g == 0, 0, jnp.where(g == 3, 1, 2))))
        e_ = jnp.where(side == 2, jnp.where(turns, g - 2, g - 1), 1)
        return side, e_, jnp.where(first, t // 2, lax.rem(t, UNITS))

    def unit_dev(side, e_):
        return jnp.where(side == 0, lchip, jnp.where(side == 1, rchip, ochip)) * 2 + e_

    def unit_pass_on(t):
        side, which, k = unit_order(t)

        @pl.when(side == 0)
        def _():
            arrived(1, k, "r1", "l1")
            start(1, k, "r3", "l3", "pl1", "pr1")

        for e_ in range(2):

            @pl.when((side == 2) & (which == e_))
            def _(e_=str(e_), over=str(e_ + 2)):
                arrived(1, k, "r" + over, "l" + over)
                start(1, k, "po" + e_)

    def unit_load(t):
        side, e_, k = unit_order(t)
        slot = lax.rem(t, 2)
        return pltpu.make_async_copy(g_ref.at[_at(unit_dev(side, e_) * tok + k * unit, unit)], chunk_s.at[0, _at(slot * unit, unit)], sem_load.at[slot, 0])

    def unit_fetch(t):
        side, which, k = unit_order(t)
        for name, test in (("pl1", side == 0), ("pr1", side == 1), ("po0", (side == 2) & (which == 0)), ("po1", (side == 2) & (which == 1))):

            @pl.when(test)
            def _(name=name):
                arrived(1, k, name)

        unit_load(t).start()

    def backward(s):
        j = order(s)
        slot = lax.rem(s, 2)

        @pl.when(s >= 2)
        def _():
            each(lambda k: load(1, s, k).wait())

        @pl.when((s == 2) | (s == 4))
        def _():
            fetch_next(1, s + 1)

        @pl.when(s >= 2)
        def _():
            keep_d_out(slot)

        total = mix_s[j, HEAD:HEAD + 1, :]
        lse_s[...] = top_s[j] * e + jnp.log2(total)
        for h in range(heads):
            out = (mix_s[j, :HEAD, strips[h]] * (1 / total[:, h * tok:(h + 1) * tok])).astype(LOW)
            turn_s[pl.ds(width + h * HEAD, HEAD), rows(j)] = out
            one = do_s[slot, strips[h], :]
            delta_s[:, strips[h]] = (one.astype(F32).T * out.astype(F32)).sum(axis=0, keepdims=True)
        dq_s[...] = jnp.zeros_like(dq_s)

        def block(i, masked):
            here = rows(i)
            scores = _dot(k_s[here, :], q_s[j], 1, 1)
            dps = _dot(v_s[here, :], do_s[slot], 1, 1)
            ps, dss = [], []
            for h, at in enumerate(strips):
                p = jnp.exp2(scores[:, h * tok:(h + 1) * tok] * e - lse_s[:, at])
                if masked:
                    p = jnp.where(visible(), p, 0.0)
                dss.append((p * (dps[:, h * tok:(h + 1) * tok] - delta_s[:, at])).astype(LOW))
                ps.append(p.astype(LOW))
            p, ds = jnp.concatenate(ps, axis=1), jnp.concatenate(dss, axis=1)
            dv_s[here, :] += _dot(p, do_s[slot], 1, 0)
            dk_s[here, :] += _dot(ds, q_s[j], 1, 0)
            dq_s[...] += _dot(kt_s[:, here], ds, 1, 0)

        lax.fori_loop(0, j, lambda i, _: block(i, False), None)

        units_next = (s == 3) & jnp.logical_not(wraps)
        whole_next = (s == 1) | (s == 5) | (s == 6) | ((s == 3) & wraps)

        @pl.when(whole_next)
        def _():
            pass_on(1, s + 1)

        @pl.when(units_next)
        def _():
            unit_pass_on(0)

        block(j, True)

        @pl.when(whole_next)
        def _():
            fetch_next(1, s + 1)

        @pl.when(units_next)
        def _():
            unit_fetch(0)

        cos, sin = tables(j)
        for h in range(heads):
            one = (dq_s[:, strips[h]] * HEAD**-0.5).T.astype(LOW).astype(F32)
            grads_s[rows(j), lanes[h]] = turned(one, cos, -sin)


    def unit_backward(t):
        side, e_, k = unit_order(t)
        j, slot = unit_dev(side, e_), lax.rem(t, 2)
        unit_load(t).wait()

        d_out = _dot(chunk_s[0, _at(slot * unit, unit), :], wo_s[...], 1, 0).astype(LOW)
        at = _at(j * tok + k * unit, unit)
        mine = [pl.ds(h * unit, unit) for h in range(heads)]
        for h in range(heads):
            lane = _at(h * tok + k * unit, unit)
            total = mix_s[j, HEAD:HEAD + 1, lane]
            out = (mix_s[j, :HEAD, lane] * (1 / total)).astype(LOW)
            turn_s[pl.ds(width + h * HEAD, HEAD), at] = out
            one = d_out[:, h * HEAD:(h + 1) * HEAD]
            do_u[mine[h], :] = one
            q_u[mine[h], :] = q_s[j, lane, :]
            delta_s[:, mine[h]] = (one.astype(F32).T * out.astype(F32)).sum(axis=0, keepdims=True)
            lse_s[:, mine[h]] = top_s[j, :, lane] * e + jnp.log2(total)
        across_u = heads * unit
        dq_s[:, :across_u] = jnp.zeros((HEAD, across_u), F32)

        def span(first, count, masked):
            here = _at(first * tok, count * tok, tok)
            scores = _dot(k_s[here, :], q_u[...], 1, 1)
            dps = _dot(v_s[here, :], do_u[...], 1, 1)
            ps, dss = [], []
            for b in range(count):
                p = jnp.exp2(scores[b * tok:(b + 1) * tok] * e - lse_s[:, :across_u])
                if masked and b == count - 1:
                    query = lax.rem(lax.broadcasted_iota(jnp.int32, (tok, across_u), 1), unit) + k * unit
                    p = jnp.where(query >= lax.broadcasted_iota(jnp.int32, (tok, across_u), 0), p, 0.0)
                dss.append((p * (dps[b * tok:(b + 1) * tok] - delta_s[:, :across_u])).astype(LOW))
                ps.append(p.astype(LOW))
            p, ds = jnp.concatenate(ps, axis=0), jnp.concatenate(dss, axis=0)
            dv_s[here, :] += _dot(p, do_u[...], 1, 0)
            dk_s[here, :] += _dot(ds, q_u[...], 1, 0)
            dq_s[:, :across_u] += _dot(kt_s[:, here], ds, 1, 0)

        most = 3
        times = j // most

        @pl.when(t + 1 < steps)
        def _():
            unit_pass_on(t + 1)

        lax.fori_loop(0, times, lambda i, _: span(i * most, most, False), None)

        @pl.when(t + 1 < steps)
        def _():
            unit_fetch(t + 1)

        for rest in range(most):

            @pl.when(j - times * most == rest)
            def _(rest=rest):
                span(j - rest, rest + 1, True)

        cos, sin = tables(j, _at(k * unit, unit))
        for h in range(heads):
            one = (dq_s[:, mine[h]] * HEAD**-0.5).T.astype(LOW).astype(F32)
            grads_s[at, lanes[h]] = turned(one, cos, -sin)

    def finish(j, _):
        cos, sin = tables(j)
        at = rows(j)
        one = (dk_s[at, :] * HEAD**-0.5).astype(LOW).astype(F32)
        grads_s[at, hw:hw + HEAD] = turned(one, cos, -sin)
        grads_s[at, hw + HEAD:] = dv_s[at, :].astype(LOW)

    wide = dim // 2

    def term(dst, dev, first, size, *adds):
        at = _at(dev * tok + first, size)

        def column(c, _):
            here = _at(c * wide, wide)
            t = _dot(grads_s[at, :], wt_s[:, here], 1, 0)
            for add in adds:
                t = t + add[:, here].astype(F32)
            dst[:, here] = t.astype(dst.dtype)

        lax.fori_loop(0, dim // wide, column, None)

    there = [ochip, rchip, lchip, chip]
    plan = [(0, 0, quarter), (0, half, quarter), (0, quarter, quarter), (0, half + quarter, quarter),
            (1, half, half), (2, 0, half), (1, 0, half), (2, half, half), (3, 0, half), (3, half, half)]

    def remote(i, src, dst, dev):
        return pltpu.make_async_remote_copy(src_ref=src, dst_ref=dst, send_sem=rsend.at[i], recv_sem=rrecv.at[i], device_id={"tp": dev}, device_id_type=MESH)

    def span_of(i):
        place, first, size = plan[i]
        return pair_s.at[place, pl.ds(first, size)]

    def out(i):
        return chunk_s.at[1, pl.ds(i * quarter, quarter)] if i < 4 else chunk_s.at[i % 4 // 2, pl.ds(i % 2 * half, half)]

    def pair(i):
        return remote(i, out(i), span_of(i), other)

    base = len(plan)
    sub = half // SUBS
    parts = [pl.ds(k * sub, sub) for k in range(SUBS)]
    ring_a = [remote(base + i, span_of(i), ring_s.at[i % 2, pl.ds(i // 2 * quarter, quarter)], (right, left)[i % 2]) for i in range(4)]
    ring_b = [remote(base + 4, span_of(4), last_s.at[0, 1], right), remote(base + 5, span_of(5), last_s.at[1, 0], left)]
    ring_c = [[remote(base + 6 + k, pair_s.at[1, pl.ds(k * sub, sub)], last_s.at[0, 0, p], right) for k, p in enumerate(parts)],
              [remote(base + 6 + SUBS + k, pair_s.at[2, pl.ds(half + k * sub, sub)], last_s.at[1, 1, p], left) for k, p in enumerate(parts)]]

    def give(i):
        place, first, size = plan[i]
        if i >= 8:
            pair(i - 4).wait_send()
        term(out(i), there[place] * 2 + 1 - core, first, size)
        pair(i).start()

    def take(i, *adds):
        place, first, size = plan[i]
        pair(i).wait_recv()
        term(span_of(i), there[place] * 2 + core, first, size, span_of(i), *adds)

    def first_terms():
        lax.fori_loop(0, 2, lambda i, _: finish(ochip * 2 + i, _), None)
        give(0)
        give(1)
        for i in range(4):
            take(i)
            ring_a[i].start()
            if i < 2:
                give(i + 2)

    whole = jnp.where(wraps, n, 4)
    break_at = jnp.where(wraps, n, 4 + pause)

    def g_step(t, _):
        @pl.when(t < whole)
        def _():
            backward(t)

        @pl.when(t == break_at)
        def _():
            first_terms()

        @pl.when((t >= whole) & (t != break_at))
        def _():
            unit_backward(t - whole - (t > break_at).astype(jnp.int32))

    lax.fori_loop(0, jnp.where(wraps, n, 4 + steps) + 1, g_step, None)
    lax.fori_loop(2, n, lambda i, _: finish(lax.rem(ochip * 2 + i, n), _), None)
    for i in range(4):
        pair(i).wait_send()
    give(4)
    give(5)
    for i in (4, 5):
        take(i)
        ring_b[i - 4].start()
    for i in range(6, 10):
        give(i)

    def lay(j, _):
        turn_s[:width, rows(j)] = grads_s[rows(j), :].T

    lax.fori_loop(0, n, lay, None)
    for i in (8, 9):
        place, first, size = plan[i]
        pair(i).wait_recv()
        term(own_s.at[pl.ds(first, size)], me, first, size, span_of(i))

    size = dw_s.shape[0]
    blocks = dim // size
    flows = [wo_s, flow_s]

    def fetch(s, kind):
        return pltpu.make_async_copy((a_ref, g_ref)[kind].at[:, _at(s * size, size)], flows[kind], sem_in.at[kind])

    def puts(s):
        at = _at(s * size, size)
        return [pltpu.make_async_copy(dw_s.at[:, :hw], by_wq_ref.at[at], sem_out.at[0]),
                pltpu.make_async_copy(dw_s.at[:, hw:hw + HEAD], by_wk_ref.at[at], sem_out.at[1]),
                pltpu.make_async_copy(dw_s.at[:, hw + HEAD:], by_wv_ref.at[at], sem_out.at[2])]

    def put_o(s):
        return pltpu.make_async_copy(dwo_s, by_wo_ref.at[:, _at(s * size, size)], sem_out.at[3])

    fetch(0, 0).start()
    fetch(0, 1).start()

    def weights(s, _):
        fetch(s, 0).wait()
        dw = _dot(turn_s[:width, :], flows[0][...], 1, 0)

        @pl.when(s + 1 < blocks)
        def _():
            fetch(s + 1, 0).start()

        @pl.when(s > 0)
        def _():
            for put in puts(s - 1):
                put.wait()

        dw_s[...] = dw.T.astype(LOW)
        for put in puts(s):
            put.start()
        fetch(s, 1).wait()
        dwo = _dot(turn_s[width:, :], flows[1][...], 1, 0)

        @pl.when(s + 1 < blocks)
        def _():
            fetch(s + 1, 1).start()

        @pl.when(s > 0)
        def _():
            put_o(s - 1).wait()

        dwo_s[...] = dwo.astype(LOW)
        put_o(s).start()

    lax.fori_loop(0, blocks // 2, weights, None)
    for h in range(2):
        for one in ring_a[h::2]:
            one.wait_recv()
        take(6 + h, ring_s.at[h])
        for one in ring_c[h]:
            one.start()
    lax.fori_loop(blocks // 2, blocks, weights, None)
    for put in puts(blocks - 1):
        put.wait()
    put_o(blocks - 1).wait()

    pulls = [pltpu.make_async_copy(x_ref.at[pl.ds(h * half, half)], pair_s.at[3, pl.ds(h * half, half)], loc.at[h]) for h in range(2)]
    pulls += [pltpu.make_async_copy(dy_ref.at[pl.ds(h * half, half)], ring_s.at[h], loc.at[2 + h]) for h in range(2)]
    for pull in pulls:
        pull.start()
    sum_s[...] = jnp.zeros_like(sum_s)
    for pull in pulls:
        pull.wait()
    for one in ring_b:
        one.wait_recv()
    step = 32

    def normal(at):
        wide_x = pair_s[3, at, :].astype(F32)
        scale = lax.rsqrt(jnp.mean(wide_x * wide_x, -1, keepdims=True) + 1e-6)
        return wide_x * scale, scale

    def total_rows(k, h):
        def some(r, _):
            at = _at(k * sub + r * step, step)
            whole = _at(h * half + k * sub + r * step, step)
            da = (own_s[whole, :] + last_s[0, h, at, :].astype(F32) + last_s[1, h, at, :].astype(F32)).astype(LOW)
            last_s[0, h, at, :] = da
            both = da.astype(F32) * normal(whole)[0]
            sum_s[...] += sum(both[i:i + 8] for i in range(0, step, 8))

        lax.fori_loop(0, sub // step, some, None)

    def x_rows(k, h):
        def some(r, _):
            at = _at(k * sub + r * step, step)
            hat, scale = normal(_at(h * half + k * sub + r * step, step))
            d_hat = last_s[0, h, at, :].astype(F32) * gain
            inner = jnp.mean(d_hat * hat, -1, keepdims=True)
            ring_s[h, at, :] = ((d_hat - hat * inner) * scale + ring_s[h, at, :].astype(F32)).astype(LOW)

        lax.fori_loop(0, sub // step, some, None)
        save = pltpu.make_async_copy(ring_s.at[h, parts[k]], dx_ref.at[pl.ds(h * half + k * sub, sub)], sem_out.at[4 + 2 * k + h])
        save.start()
        return save

    def swap(k, dev, owner):
        line = gain_s.at[owner]
        return pltpu.make_async_remote_copy(src_ref=line, dst_ref=line, send_sem=gsend.at[k - 1], recv_sem=grecv.at[k - 1], device_id={"tp": dev}, device_id_type=MESH)

    saves = []
    for k in range(SUBS):
        for h in range(2):
            ring_c[h][k].wait_recv()
            total_rows(k, h)
        if k == SUBS - 1:
            gain_s[me] = sum_s[...].sum(axis=0, keepdims=True)
            for i in range(1, n):
                swap(i, lax.rem(me + i, n), me).start()
        saves += [x_rows(k, h) for h in range(2)]
    for k in range(1, n):
        swap(k, other, lax.rem(me + n - k, n)).wait_recv()
    by_gain_ref[...] = sum(gain_s[k] for k in range(n))
    for k in range(1, n):
        swap(k, lax.rem(me + k, n), me).wait_send()
    for z in range(2):
        def sent_full(i, _, z=z):
            first = a_ref.at[pl.ds(0, 2 * few)]
            pltpu.make_async_remote_copy(src_ref=first, dst_ref=first, send_sem=send.at[z, i], recv_sem=recv.at[z, i], device_id={"tp": other}, device_id_type=MESH).wait_send()

        def sent_few(i, _, z=z):
            first = a_ref.at[pl.ds(0, few)]
            pltpu.make_async_remote_copy(src_ref=first, dst_ref=first, send_sem=send.at[z, i], recv_sem=recv.at[z, i], device_id={"tp": other}, device_id_type=MESH).wait_send()

        lax.fori_loop(0, 4 * UNITS, sent_full, None)
        lax.fori_loop(6 * UNITS, full_pieces * UNITS, sent_full, None)
        lax.fori_loop(full_pieces * UNITS, len(pieces) * UNITS, sent_few, None)
    for i in range(6, 10):
        pair(i).wait_send()
    for one in [*ring_a, *ring_b, *ring_c[0], *ring_c[1]]:
        one.wait_send()
    for save in saves:
        save.wait()


def _results(*refs):
    k = len(refs) // 3
    sources, targets, rooms = refs[:k], refs[k:2 * k], refs[2 * k:3 * k]
    into, out = refs[-2:]
    pulls = [pltpu.make_async_copy(a, b, into.at[i]) for i, (a, b) in enumerate(zip(sources, rooms))]
    puts = [pltpu.make_async_copy(a, b, out.at[i]) for i, (a, b) in enumerate(zip(rooms, targets))]
    for pull in pulls:
        pull.start()
    for pull, put in zip(pulls, puts):
        pull.wait()
        put.start()
    for put in puts:
        put.wait()


def solution(mesh):
    n = mesh.shape["tp"]

    def step(x, dy, gain, wq, wk, wv, wo):
        tok, dim = x.shape
        heads = wq.shape[1] // HEAD
        hw = heads * HEAD
        width = hw + 2 * HEAD
        rows, cols, half = n * tok, heads * tok, tok // 2
        freq = np.float64(THETA) ** (-np.arange(HEAD // 2) / (HEAD // 2))

        def table(places):
            angle = np.asarray(places, np.float64)[:, None] * freq
            cos, sin = np.cos(angle), np.sin(angle)
            return jnp.asarray(np.stack([np.concatenate([cos, cos], 1), np.concatenate([-sin, sin], 1)]), F32)

        near, far = table(np.arange(tok)), table(np.arange(n) * tok)
        anywhere, vmem = pl.BlockSpec(memory_space=pl.ANY), pl.BlockSpec(memory_space=pltpu.VMEM)
        dma, scratch, shape = pltpu.SemaphoreType.DMA, pltpu.VMEM, jax.ShapeDtypeStruct
        size = hw
        most = max(rows, dim)
        ring = 16 + 2 * SUBS
        sends = 16 * UNITS
        _, _, *results = pl.pallas_call(
            functools.partial(_kernel, n, heads),
            out_shape=[shape((rows, dim), LOW), shape((rows, dim), LOW), shape((tok, dim), LOW), shape((1, dim), F32),
                       shape(wq.shape, LOW), shape(wk.shape, LOW), shape(wv.shape, LOW), shape(wo.shape, LOW)],
            in_specs=[anywhere, anywhere, vmem, anywhere, anywhere, anywhere, anywhere, vmem, vmem],
            out_specs=[anywhere, anywhere, anywhere, vmem, anywhere, anywhere, anywhere, anywhere],
            scratch_shapes=[
                scratch((2, tok, dim), LOW), scratch((width, dim), LOW), scratch((most, hw), LOW),
                scratch((n, cols, HEAD), LOW), scratch((most, HEAD), LOW), scratch((HEAD, rows), LOW), scratch((most, HEAD), LOW), scratch((HEAD + 8, rows), LOW),
                scratch((1, cols), F32), scratch((2, cols, HEAD), LOW), scratch((cols // UNITS, HEAD), LOW), scratch((cols // UNITS, HEAD), LOW), scratch((1, cols), F32), scratch((n, 1, cols), F32), scratch((n, HEAD + 8, cols), F32),
                scratch((HEAD, cols), F32), scratch((rows, HEAD), F32), scratch((rows, HEAD), F32), scratch((rows, width), LOW), scratch((width + hw, rows), LOW),
                scratch((4, tok, dim), LOW), scratch((2, half, dim), LOW), scratch((2, 2, half, dim), LOW), scratch((tok, dim), F32),
                scratch((most, size), LOW), scratch((size, width), LOW), scratch((hw, size), LOW), scratch((n, 1, dim), F32), scratch((8, dim), F32),
                dma((2, sends)), dma((2, sends)), dma((ring,)), dma((ring,)), dma((n - 1,)), dma((n - 1,)), dma((5,)), dma((dim // hw,)), dma((2, UNITS)), dma((2,)), dma((4 + 2 * SUBS,))],
            compiler_params=pltpu.CompilerParams(collective_id=0, has_side_effects=True, vmem_limit_bytes=VMEM),
            name="layer",
        )(x, dy, gain, wq, wk, wv, wo, near, far)
        kept = [results[i] for i in (2, 3, 4, 0, 5, 1)]
        out = pl.pallas_call(
            _results,
            out_shape=[shape(t.shape, t.dtype) for t in kept],
            in_specs=[anywhere] * len(kept),
            out_specs=[anywhere] * len(kept),
            scratch_shapes=[*[scratch(t.shape, t.dtype) for t in kept], dma((len(kept),)), dma((len(kept),))],
            compiler_params=pltpu.CompilerParams(vmem_limit_bytes=VMEM),
            name="results",
        )(*kept)
        return out[3], out[5], out[0], out[1], out[2], out[4]

    tokens, columns = P(("dp", "tp"), None), P(None, "tp")
    return jax.shard_map(
        step,
        mesh=mesh,
        in_specs=(tokens, tokens, P(None), columns, columns, columns, P("tp", None)),
        out_specs=(tokens, P("dp", None), P("dp", "tp"), P("dp", "tp"), P("dp", "tp"), P(("dp", "tp"), None)),
        check_vma=False,
    )
```

```python
import functools

import jax
import jax.numpy as jnp
import numpy as np
from jax import lax
from jax.experimental import pallas as pl
from jax.experimental.pallas import tpu as pltpu
from jax.sharding import PartitionSpec as P

HEAD = 128
THETA = 10000
NEG = -1e30
HIDDEN = 2 * NEG
LOG2E = 1.4426950408889634
VMEM = 67_043_328
MESH = pl.DeviceIdType.MESH
F32, LOW = jnp.float32, jnp.bfloat16
UNITS = 3
SUBS = 3


def _dot(a, b, ca, cb):
    return lax.dot_general(a, b, (((ca,), (cb,)), ((), ())), preferred_element_type=F32)


def _at(start, size, unit=None):
    return pl.ds(pl.multiple_of(start, unit or size), size)


def _kernel(n, heads, x_ref, dy_ref, gain_ref, wq_ref, wk_ref, wv_ref, wo_ref, near_ref, far_ref,
            a_ref, g_ref, dx_ref, by_gain_ref, by_wq_ref, by_wk_ref, by_wv_ref, by_wo_ref,
            chunk_s, wt_s, wo_s, q_s, k_s, kt_s, v_s, vt_s, lse_s, do_s, do_u, delta_s, top_s, mix_s, dq_s, dk_s, dv_s, grads_s, turn_s,
            pair_s, ring_s, last_s, own_s, flow_s, gain_s, sum_s, send, recv, rsend, rrecv, gsend, grecv, loc, sem_wo, sem_load, sem_in, sem_out):
    tok, dim = x_ref.shape
    half, quarter, hw = tok // 2, tok // 4, heads * HEAD
    unit = tok // UNITS
    width = hw + 2 * HEAD
    chips = n // 2
    me = lax.axis_index("tp")
    chip, core = me // 2, lax.rem(me, 2)
    other = chip * 2 + 1 - core
    lchip, rchip, ochip = lax.rem(chip + chips - 1, chips), lax.rem(chip + 1, chips), lax.rem(chip + chips // 2, chips)
    left, right, across = lchip * 2 + core, rchip * 2 + core, ochip * 2 + core
    e = HEAD**-0.5 * LOG2E

    few = unit // 4

    def part(c):
        return unit // 2 * c

    away = 1 - core
    pieces = {}

    def piece(name, sent, got, to, size=2 * few):
        pieces[name] = (len(pieces) * UNITS, sent, got, to, size)

    for name, to, c_from in (("r", right, lchip), ("l", left, rchip)):
        for k in range(2):
            piece(name + str(k), (chip, k, part(core)), (c_from, k, part(core)), to)
    piece("p", (chip, core, part(away)), (chip, away, part(core)), other)
    piece("q", (chip, core, part(core)), (chip, away, part(away)), other)
    for name, c in (("pl", lchip), ("pr", rchip), ("po", ochip)):
        for k in range(2):
            piece(name + str(k), (c, k, part(core)), (c, k, part(away)), other)
    full_pieces = len(pieces)
    for name, to, c_over, shift in (("r", right, lchip, 0), ("l", left, rchip, few)):
        for k in range(2):
            piece(name + str(k + 2), (c_over, k, part(core) + shift), (ochip, k, part(core) + shift), to, few)

    def each(do):
        lax.fori_loop(0, UNITS, lambda k, _: do(k), None)

    def rows(dev):
        return _at(dev * tok, tok)

    def copy(z, name, k, sending=True):
        i, sent, got, to, size = pieces[name]
        c, e_, first = sent if sending else got
        at = first + unit * k
        full = (a_ref, g_ref)[z].at[_at((c * 2 + e_) * tok + at, size, few)]
        own = name in ("p", "q")
        return pltpu.make_async_remote_copy(src_ref=chunk_s.at[z, _at(at, size, few)] if own else full, dst_ref=full,
                                            send_sem=send.at[z, i + k], recv_sem=recv.at[z, i + k], device_id={"tp": to}, device_id_type=MESH)

    def start(z, k, *names):
        for name in names:
            copy(z, name, k).start()

    def arrived(z, k, *names):
        for name in names:
            copy(z, name, k, False).wait_recv()

    def order(s):
        t = s // 2
        middle, final = (t + 1) // 2 - 2 * (t // 3), t // 3
        c = lax.rem(chip + middle * (chips - 1 - (chips - 2) * lax.rem(s, 2)) + final * (chips // 2), chips)
        k = (1 - middle - final) * lax.rem(core + s, 2) + middle * (t - 1) + final * lax.rem(s, 2)
        return c * 2 + k

    def load(z, s, k):
        dev, slot = order(s), lax.rem(s, 2)
        return pltpu.make_async_copy((a_ref, g_ref)[z].at[_at(dev * tok + k * unit, unit)], chunk_s.at[slot, _at(k * unit, unit)], sem_load.at[slot, k])

    def pass_on(z, s):
        for e_ in range(2):

            @pl.when(s == 2 + 2 * e_)
            def _(e_=str(e_), over=str(e_ + 2)):
                def one(k):
                    arrived(z, k, "r" + e_, "l" + e_)
                    start(z, k, "r" + over, "l" + over, "pl" + e_, "pr" + e_)

                def rest(k):
                    arrived(z, k, "pl" + e_)
                    load(z, s, k).start()

                def both(k):
                    one(k)
                    rest(k)

                if z == 1:
                    each(one)
                    return

                lax.fori_loop(0, UNITS - 1, lambda k, _: both(k), None)
                one(UNITS - 1)
                if z == 0 and e_ == "1":
                    each(lambda k: start(1, k, "r0", "l0"))
                    each(lambda k: start(1, k, "r1", "l1"))
                rest(UNITS - 1)

            @pl.when(s == 6 + e_)
            def _(e_=str(e_), over=str(e_ + 2)):
                def one(k):
                    arrived(z, k, "r" + over, "l" + over)
                    start(z, k, "po" + e_)

                each(one)

    def fetch_next(z, s):
        for step, name in ((3, "pr0"), (5, "pr1"), (6, "po0"), (7, "po1")):

            @pl.when(s == step)
            def _(name=name):
                each(lambda k: arrived(z, k, name))

        if z == 1:

            @pl.when(s == 2)
            def _():
                each(lambda k: arrived(z, k, "pl0"))

            @pl.when(s == 4)
            def _():
                each(lambda k: arrived(z, k, "pl1"))

            each(lambda k: load(z, s, k).start())
            return

        @pl.when((s < n) & (s != 2) & (s != 4))
        def _():
            each(lambda k: load(z, s, k).start())

    loads_x = [pltpu.make_async_copy(x_ref.at[pl.ds(k * unit, unit)], chunk_s.at[0, pl.ds(k * unit, unit)], sem_load.at[0, k]) for k in range(UNITS)]
    for one in loads_x:
        one.start()
    load_dy = pltpu.make_async_copy(dy_ref, chunk_s.at[1], loc.at[1])
    load_dy.start()
    loads = [pltpu.make_async_copy(wq_ref, flow_s, loc.at[2]), pltpu.make_async_copy(wk_ref, k_s, loc.at[3]), pltpu.make_async_copy(wv_ref, v_s, loc.at[4])]
    for one in loads:
        one.start()
    loads += [pltpu.make_async_copy(wo_ref.at[:, pl.ds(i * hw, hw)], wo_s.at[pl.ds(i * hw, hw)], sem_wo.at[i]) for i in range(dim // hw)]
    for one in loads[3:]:
        one.start()
    barrier = pltpu.get_barrier_semaphore()
    for k in range(1, n):
        pl.semaphore_signal(barrier, inc=1, device_id={"tp": lax.rem(me + k, n)}, device_id_type=MESH)

    gain = gain_ref[...].reshape(1, dim).astype(F32)
    block = 32

    def norm(r, _):
        at = _at(r * block, block)
        wide = chunk_s[0, at, :].astype(F32)
        scale = lax.rsqrt(jnp.mean(wide * wide, -1, keepdims=True) + 1e-6)
        chunk_s[0, at, :] = (wide * scale * gain).astype(LOW)

    for k, one in enumerate(loads_x):
        one.wait()
        lax.fori_loop(k * unit // block, (k + 1) * unit // block, norm, None)
        if k == 0:
            pl.semaphore_wait(barrier, n - 1)
        start(0, k, "p")
    each(lambda k: start(0, k, "q"))
    keep = pltpu.make_async_copy(chunk_s.at[0], a_ref.at[rows(me)], loc.at[0])
    keep.start()
    load_dy.wait()
    keep_dy = pltpu.make_async_copy(chunk_s.at[1], g_ref.at[rows(me)], loc.at[1])
    keep_dy.start()
    keep.wait()
    each(lambda k: arrived(0, k, "p"))
    each(lambda k: start(0, k, "r0", "l0"))
    each(lambda k: start(0, k, "r1", "l1"))
    each(lambda k: start(1, k, "p", "q"))
    keep_dy.wait()
    for one in loads:
        one.wait()

    def lay_weights(i, _):
        at = _at(i * tok, tok)
        wt_s[:hw, at] = flow_s[at, :].T
        wt_s[hw:hw + HEAD, at] = k_s[at, :].T
        wt_s[hw + HEAD:, at] = v_s[at, :].T

    def lay_wo(i, _):
        at = _at(i * hw, hw)
        wo_s[at, :] = wo_s[at, :].T

    lax.fori_loop(0, dim // tok, lay_weights, None)
    lax.fori_loop(0, dim // hw, lay_wo, None)
    each(lambda k: arrived(0, k, "q"))
    each(lambda k: arrived(1, k, "p", "q"))
    for z in range(2):
        each(lambda k, z=z: [copy(z, name, k).wait_send() for name in ("p", "q")] and None)

    cols = heads * tok
    side_by = heads * unit
    groups = [pl.ds(k * side_by, side_by) for k in range(UNITS)]

    def spot(h, k):
        return pl.ds(k * side_by + h * unit, unit)

    lanes = [pl.ds(h * HEAD, HEAD) for h in range(heads)]

    def tables(j, at=slice(None)):
        ca, sa = near_ref[0, at, :], near_ref[1, at, :]
        cb, sb = far_ref[0, pl.ds(j, 1), :], far_ref[1, pl.ds(j, 1), :]
        return ca * cb - sa * sb, sa * cb + ca * sb

    def turned(t, cos, sin):
        return (t * cos + pltpu.roll(t, HEAD // 2, 1) * sin).astype(LOW)

    def project(j, slot):
        y = _dot(chunk_s[slot], wt_s[...], 1, 1).astype(LOW).astype(F32)
        cos, sin = tables(j)
        at = rows(j)
        for h in range(heads):
            q = turned(y[:, h * HEAD:(h + 1) * HEAD], cos, sin)
            for k in range(UNITS):
                q_s[j, spot(h, k), :] = q[k * unit:(k + 1) * unit]
        k = turned(y[:, hw:hw + HEAD], cos, sin)
        v = y[:, hw + HEAD:].astype(LOW)
        k_s[at, :] = k
        kt_s[:, at] = k.T
        v_s[at, :] = v
        vt_s[:HEAD, at] = v.T

    def visible(k, more=0):
        shape = ((k + 1) * unit + more, side_by)
        return lax.rem(lax.broadcasted_iota(jnp.int32, shape, 1), unit) + k * unit >= lax.broadcasted_iota(jnp.int32, shape, 0)

    def blocks_of(j, i, masked):
        return [(k, at, pl.ds(pl.multiple_of(i * tok, tok), (k + 1) * unit if masked else tok)) for k, at in enumerate(groups)]

    def seen_block(j, i, masked):
        parts_of = blocks_of(j, i, masked)
        if masked:
            scores = [_dot(k_s[here, :], q_s[j, at, :], 1, 1) for _, at, here in parts_of]
        else:
            wide = _dot(k_s[parts_of[0][2], :], q_s[j], 1, 1)
            scores = [wide[:, k * side_by:(k + 1) * side_by] for k in range(UNITS)]
        weights, keeps = [], []
        for (k, at, _), s in zip(parts_of, scores):
            if masked:
                s = jnp.where(visible(k), s, HIDDEN)
            old = top_s[j, :, at]
            top = jnp.maximum(old, s.max(axis=0, keepdims=True))
            top_s[j, :, at] = top
            weights.append(jnp.exp2((s - top) * e).astype(LOW))
            keeps.append(jnp.exp2((old - top) * e))
        for (_, at, here), p, kept in zip(parts_of, weights, keeps):
            mix_s[j, :, at] = mix_s[j, :, at] * kept + _dot(vt_s[:, here], p, 1, 0)

    vt_s[HEAD:, :] = jnp.ones((8, n * tok), LOW)

    def clear(j, _):
        top_s[j] = jnp.full((1, cols), NEG, F32)
        mix_s[j] = jnp.zeros((HEAD + 8, cols), F32)

    lax.fori_loop(0, n, clear, None)
    dk_s[...] = jnp.zeros_like(dk_s)
    dv_s[...] = jnp.zeros_like(dv_s)

    def keep_d_out(slot):
        d_out = _dot(chunk_s[slot], wo_s[...], 1, 0).astype(LOW)
        for h in range(heads):
            for k in range(UNITS):
                do_s[slot, spot(h, k), :] = d_out[k * unit:(k + 1) * unit, h * HEAD:(h + 1) * HEAD]

    def x_step(s, _):
        j = order(s)
        early = (lax.rem(s, 2) == 0) & (s < 6)
        middle = (s == 5) | (s == 6)

        @pl.when(s > 0)
        def _():
            each(lambda k: load(0, s, k).wait())

        @pl.when(early)
        def _():
            fetch_next(0, s + 1)

        project(j, lax.rem(s, 2))

        seen_block(j, j, True)

        def earlier(t, _):
            @pl.when(middle & (t == 2 * (s - 5)))
            def _():
                pass_on(0, s + 1)

            @pl.when(middle & (t == 2 * (s - 4)))
            def _():
                fetch_next(0, s + 1)

            i = order(t)
            seen_block(jnp.maximum(i, j), jnp.minimum(i, j), False)

        lax.fori_loop(0, s, earlier, None)

        @pl.when(s == 1)
        def _():
            for t in range(2):
                each(lambda k, t=t: load(1, t, k).start())

            def one(t, _):
                each(lambda k: load(1, t, k).wait())
                keep_d_out(t)

            lax.fori_loop(0, 2, one, None)

        @pl.when((s == 1) | (s == 3))
        def _():
            pass_on(0, s + 1)
            fetch_next(0, s + 1)

    lax.fori_loop(0, n, x_step, None)


    steps = 4 * UNITS
    wraps = rchip > ochip
    turns = ochip == chips - 1
    pause = jnp.where(turns, steps, steps - UNITS)

    def unit_order(t):
        g = t // UNITS
        first = turns & (g < 2)
        side = jnp.where(first, lax.rem(t, 2), jnp.where(turns, 2, jnp.where(g == 0, 0, jnp.where(g == 3, 1, 2))))
        e_ = jnp.where(side == 2, jnp.where(turns, g - 2, g - 1), 1)
        return side, e_, jnp.where(first, t // 2, lax.rem(t, UNITS))

    def unit_dev(side, e_):
        return jnp.where(side == 0, lchip, jnp.where(side == 1, rchip, ochip)) * 2 + e_

    def unit_pass_on(t):
        side, which, k = unit_order(t)

        @pl.when(side == 0)
        def _():
            arrived(1, k, "r1", "l1")
            start(1, k, "r3", "l3", "pl1", "pr1")

        for e_ in range(2):

            @pl.when((side == 2) & (which == e_))
            def _(e_=str(e_), over=str(e_ + 2)):
                arrived(1, k, "r" + over, "l" + over)
                start(1, k, "po" + e_)

    def unit_load(t):
        side, e_, k = unit_order(t)
        slot = lax.rem(t, 2)
        return pltpu.make_async_copy(g_ref.at[_at(unit_dev(side, e_) * tok + k * unit, unit)], chunk_s.at[0, _at(slot * unit, unit)], sem_load.at[slot, 0])

    def unit_fetch(t):
        side, which, k = unit_order(t)
        for name, test in (("pl1", side == 0), ("pr1", side == 1), ("po0", (side == 2) & (which == 0)), ("po1", (side == 2) & (which == 1))):

            @pl.when(test)
            def _(name=name):
                arrived(1, k, name)

        unit_load(t).start()

    def backward(s):
        j = order(s)
        slot = lax.rem(s, 2)

        @pl.when(s >= 2)
        def _():
            each(lambda k: load(1, s, k).wait())

        @pl.when((s == 2) | (s == 4))
        def _():
            fetch_next(1, s + 1)

        @pl.when(s >= 2)
        def _():
            keep_d_out(slot)

        total = mix_s[j, HEAD:HEAD + 1, :]
        lse_s[...] = top_s[j] * e + jnp.log2(total)
        for h in range(heads):
            for k in range(UNITS):
                at = spot(h, k)
                out = (mix_s[j, :HEAD, at] * (1 / total[:, k * side_by + h * unit:k * side_by + (h + 1) * unit])).astype(LOW)
                turn_s[pl.ds(width + h * HEAD, HEAD), _at(j * tok + k * unit, unit)] = out
                delta_s[:, at] = (do_s[slot, at, :].astype(F32).T * out.astype(F32)).sum(axis=0, keepdims=True)
        dq_s[...] = jnp.zeros_like(dq_s)

        def block(i):
            here = rows(i)
            scores = _dot(k_s[here, :], q_s[j], 1, 1)
            dps = _dot(v_s[here, :], do_s[slot], 1, 1)
            ps, dss = [], []
            for k, at in enumerate(groups):
                p = jnp.exp2(scores[:, k * side_by:(k + 1) * side_by] * e - lse_s[:, at])
                dss.append((p * (dps[:, k * side_by:(k + 1) * side_by] - delta_s[:, at])).astype(LOW))
                ps.append(p.astype(LOW))
            p, ds = jnp.concatenate(ps, axis=1), jnp.concatenate(dss, axis=1)
            dv_s[here, :] += _dot(p, do_s[slot], 1, 0)
            dk_s[here, :] += _dot(ds, q_s[j], 1, 0)
            dq_s[...] += _dot(kt_s[:, here], ds, 1, 0)

        def own_block():
            parts_of = blocks_of(j, j, True)
            scores = [_dot(k_s[here, :], q_s[j, at, :], 1, 1) for _, at, here in parts_of]
            dps = [_dot(v_s[here, :], do_s[slot, at, :], 1, 1) for _, at, here in parts_of]
            for (k, at, here), sc, dp in zip(parts_of, scores, dps):
                p = jnp.where(visible(k), jnp.exp2(sc * e - lse_s[:, at]), 0.0)
                ds = (p * (dp - delta_s[:, at])).astype(LOW)
                dv_s[here, :] += _dot(p.astype(LOW), do_s[slot, at, :], 1, 0)
                dk_s[here, :] += _dot(ds, q_s[j, at, :], 1, 0)
                dq_s[:, at] += _dot(kt_s[:, here], ds, 1, 0)

        lax.fori_loop(0, j, lambda i, _: block(i), None)

        units_next = (s == 3) & jnp.logical_not(wraps)
        whole_next = (s == 1) | (s == 5) | (s == 6) | ((s == 3) & wraps)

        @pl.when(whole_next)
        def _():
            pass_on(1, s + 1)

        @pl.when(units_next)
        def _():
            unit_pass_on(0)

        own_block()

        @pl.when(whole_next)
        def _():
            fetch_next(1, s + 1)

        @pl.when(units_next)
        def _():
            unit_fetch(0)

        cos, sin = tables(j)
        for h in range(heads):
            whole_dq = jnp.concatenate([dq_s[:, spot(h, k)] for k in range(UNITS)], axis=1)
            one = (whole_dq * HEAD**-0.5).T.astype(LOW).astype(F32)
            grads_s[rows(j), lanes[h]] = turned(one, cos, -sin)


    def unit_backward(t):
        side, e_, k = unit_order(t)
        j, slot = unit_dev(side, e_), lax.rem(t, 2)
        unit_load(t).wait()

        d_out = _dot(chunk_s[0, _at(slot * unit, unit), :], wo_s[...], 1, 0).astype(LOW)
        at = _at(j * tok + k * unit, unit)
        mine = [pl.ds(h * unit, unit) for h in range(heads)]
        for h in range(heads):
            lane = _at(k * side_by + h * unit, unit)
            total = mix_s[j, HEAD:HEAD + 1, lane]
            out = (mix_s[j, :HEAD, lane] * (1 / total)).astype(LOW)
            turn_s[pl.ds(width + h * HEAD, HEAD), at] = out
            one = d_out[:, h * HEAD:(h + 1) * HEAD]
            do_u[mine[h], :] = one
            delta_s[:, mine[h]] = (one.astype(F32).T * out.astype(F32)).sum(axis=0, keepdims=True)
            lse_s[:, mine[h]] = top_s[j, :, lane] * e + jnp.log2(total)
        across_u = side_by
        q_u = q_s.at[j, _at(k * side_by, side_by)]
        dq_s[:, :across_u] = jnp.zeros((HEAD, across_u), F32)

        def span(first, count, masked):
            here = _at(first * tok, count * tok, tok)
            scores = _dot(k_s[here, :], q_u[...], 1, 1)
            dps = _dot(v_s[here, :], do_u[...], 1, 1)
            ps, dss = [], []
            for b in range(count):
                p = jnp.exp2(scores[b * tok:(b + 1) * tok] * e - lse_s[:, :across_u])
                if masked and b == count - 1:
                    query = lax.rem(lax.broadcasted_iota(jnp.int32, (tok, across_u), 1), unit) + k * unit
                    p = jnp.where(query >= lax.broadcasted_iota(jnp.int32, (tok, across_u), 0), p, 0.0)
                dss.append((p * (dps[b * tok:(b + 1) * tok] - delta_s[:, :across_u])).astype(LOW))
                ps.append(p.astype(LOW))
            p, ds = jnp.concatenate(ps, axis=0), jnp.concatenate(dss, axis=0)
            dv_s[here, :] += _dot(p, do_u[...], 1, 0)
            dk_s[here, :] += _dot(ds, q_u[...], 1, 0)
            dq_s[:, :across_u] += _dot(kt_s[:, here], ds, 1, 0)

        most = 3
        times = j // most

        @pl.when(t + 1 < steps)
        def _():
            unit_pass_on(t + 1)

        lax.fori_loop(0, times, lambda i, _: span(i * most, most, False), None)

        @pl.when(t + 1 < steps)
        def _():
            unit_fetch(t + 1)

        for rest in range(most):

            @pl.when(j - times * most == rest)
            def _(rest=rest):
                span(j - rest, rest + 1, True)

        cos, sin = tables(j, _at(k * unit, unit))
        for h in range(heads):
            one = (dq_s[:, mine[h]] * HEAD**-0.5).T.astype(LOW).astype(F32)
            grads_s[at, lanes[h]] = turned(one, cos, -sin)

    def finish(j, _):
        cos, sin = tables(j)
        at = rows(j)
        one = (dk_s[at, :] * HEAD**-0.5).astype(LOW).astype(F32)
        grads_s[at, hw:hw + HEAD] = turned(one, cos, -sin)
        grads_s[at, hw + HEAD:] = dv_s[at, :].astype(LOW)

    wide = dim // 2

    def term(dst, dev, first, size, *adds):
        at = _at(dev * tok + first, size)

        def column(c, _):
            here = _at(c * wide, wide)
            t = _dot(grads_s[at, :], wt_s[:, here], 1, 0)
            for add in adds:
                t = t + add[:, here].astype(F32)
            dst[:, here] = t.astype(dst.dtype)

        lax.fori_loop(0, dim // wide, column, None)

    there = [ochip, rchip, lchip, chip]
    plan = [(0, 0, quarter), (0, half, quarter), (0, quarter, quarter), (0, half + quarter, quarter),
            (1, half, half), (2, 0, half), (1, 0, half), (2, half, half), (3, 0, half), (3, half, half)]

    def remote(i, src, dst, dev):
        return pltpu.make_async_remote_copy(src_ref=src, dst_ref=dst, send_sem=rsend.at[i], recv_sem=rrecv.at[i], device_id={"tp": dev}, device_id_type=MESH)

    def span_of(i):
        place, first, size = plan[i]
        return pair_s.at[place, pl.ds(first, size)]

    def out(i):
        return chunk_s.at[1, pl.ds(i * quarter, quarter)] if i < 4 else chunk_s.at[i % 4 // 2, pl.ds(i % 2 * half, half)]

    def pair(i):
        return remote(i, out(i), span_of(i), other)

    base = len(plan)
    sub = half // SUBS
    parts = [pl.ds(k * sub, sub) for k in range(SUBS)]
    ring_a = [remote(base + i, span_of(i), ring_s.at[i % 2, pl.ds(i // 2 * quarter, quarter)], (right, left)[i % 2]) for i in range(4)]
    ring_b = [remote(base + 4, span_of(4), last_s.at[0, 1], right), remote(base + 5, span_of(5), last_s.at[1, 0], left)]
    ring_c = [[remote(base + 6 + k, pair_s.at[1, pl.ds(k * sub, sub)], last_s.at[0, 0, p], right) for k, p in enumerate(parts)],
              [remote(base + 6 + SUBS + k, pair_s.at[2, pl.ds(half + k * sub, sub)], last_s.at[1, 1, p], left) for k, p in enumerate(parts)]]

    def give(i):
        place, first, size = plan[i]
        if i >= 8:
            pair(i - 4).wait_send()
        term(out(i), there[place] * 2 + 1 - core, first, size)
        pair(i).start()

    def take(i, *adds):
        place, first, size = plan[i]
        pair(i).wait_recv()
        term(span_of(i), there[place] * 2 + core, first, size, span_of(i), *adds)

    def first_terms():
        lax.fori_loop(0, 2, lambda i, _: finish(ochip * 2 + i, _), None)
        give(0)
        give(1)
        for i in range(4):
            take(i)
            ring_a[i].start()
            if i < 2:
                give(i + 2)

    whole = jnp.where(wraps, n, 4)
    break_at = jnp.where(wraps, n, 4 + pause)

    def g_step(t, _):
        @pl.when(t < whole)
        def _():
            backward(t)

        @pl.when(t == break_at)
        def _():
            first_terms()

        @pl.when((t >= whole) & (t != break_at))
        def _():
            unit_backward(t - whole - (t > break_at).astype(jnp.int32))

    lax.fori_loop(0, jnp.where(wraps, n, 4 + steps) + 1, g_step, None)
    lax.fori_loop(2, n, lambda i, _: finish(lax.rem(ochip * 2 + i, n), _), None)
    for i in range(4):
        pair(i).wait_send()
    give(4)
    give(5)
    for i in (4, 5):
        take(i)
        ring_b[i - 4].start()
    for i in range(6, 10):
        give(i)

    def lay(j, _):
        turn_s[:width, rows(j)] = grads_s[rows(j), :].T

    lax.fori_loop(0, n, lay, None)
    for i in (8, 9):
        place, first, size = plan[i]
        pair(i).wait_recv()
        term(own_s.at[pl.ds(first, size)], me, first, size, span_of(i))

    for i in range(6, 10):
        pair(i).wait_send()
    size = hw
    dw_s, dwo_s = chunk_s.at[0, pl.ds(0, size), pl.ds(0, width)], chunk_s.at[1, pl.ds(0, hw), pl.ds(0, size)]
    blocks = dim // size
    flows = [wo_s, flow_s]

    def fetch(s, kind):
        return pltpu.make_async_copy((a_ref, g_ref)[kind].at[:, _at(s * size, size)], flows[kind], sem_in.at[kind])

    def puts(s):
        at = _at(s * size, size)
        return [pltpu.make_async_copy(dw_s.at[:, :hw], by_wq_ref.at[at], sem_out.at[0]),
                pltpu.make_async_copy(dw_s.at[:, hw:hw + HEAD], by_wk_ref.at[at], sem_out.at[1]),
                pltpu.make_async_copy(dw_s.at[:, hw + HEAD:], by_wv_ref.at[at], sem_out.at[2])]

    def put_o(s):
        return pltpu.make_async_copy(dwo_s, by_wo_ref.at[:, _at(s * size, size)], sem_out.at[3])

    fetch(0, 0).start()
    fetch(0, 1).start()

    def weights(s, _):
        fetch(s, 0).wait()
        dw = _dot(turn_s[:width, :], flows[0][...], 1, 0)

        @pl.when(s + 1 < blocks)
        def _():
            fetch(s + 1, 0).start()

        @pl.when(s > 0)
        def _():
            for put in puts(s - 1):
                put.wait()

        dw_s[...] = dw.T.astype(LOW)
        for put in puts(s):
            put.start()
        fetch(s, 1).wait()
        dwo = _dot(turn_s[width:, :], flows[1][...], 1, 0)

        @pl.when(s + 1 < blocks)
        def _():
            fetch(s + 1, 1).start()

        @pl.when(s > 0)
        def _():
            put_o(s - 1).wait()

        dwo_s[...] = dwo.astype(LOW)
        put_o(s).start()

    lax.fori_loop(0, blocks // 2, weights, None)
    for h in range(2):
        for one in ring_a[h::2]:
            one.wait_recv()
        take(6 + h, ring_s.at[h])
        for one in ring_c[h]:
            one.start()
    for z in range(2):
        def sent_full(i, _, z=z):
            first = a_ref.at[pl.ds(0, 2 * few)]
            pltpu.make_async_remote_copy(src_ref=first, dst_ref=first, send_sem=send.at[z, i], recv_sem=recv.at[z, i], device_id={"tp": other}, device_id_type=MESH).wait_send()

        def sent_few(i, _, z=z):
            first = a_ref.at[pl.ds(0, few)]
            pltpu.make_async_remote_copy(src_ref=first, dst_ref=first, send_sem=send.at[z, i], recv_sem=recv.at[z, i], device_id={"tp": other}, device_id_type=MESH).wait_send()

        lax.fori_loop(0, 4 * UNITS, sent_full, None)
        lax.fori_loop(6 * UNITS, full_pieces * UNITS, sent_full, None)
        lax.fori_loop(full_pieces * UNITS, len(pieces) * UNITS, sent_few, None)
    lax.fori_loop(blocks // 2, blocks, weights, None)
    for put in puts(blocks - 1):
        put.wait()
    put_o(blocks - 1).wait()

    pulls = [pltpu.make_async_copy(x_ref.at[pl.ds(h * half, half)], pair_s.at[3, pl.ds(h * half, half)], loc.at[h]) for h in range(2)]
    pulls += [pltpu.make_async_copy(dy_ref.at[pl.ds(h * half, half)], ring_s.at[h], loc.at[2 + h]) for h in range(2)]
    for pull in pulls:
        pull.start()
    sum_s[...] = jnp.zeros_like(sum_s)
    for pull in pulls:
        pull.wait()
    for one in ring_b:
        one.wait_recv()
    step = 32

    def normal(at):
        wide_x = pair_s[3, at, :].astype(F32)
        scale = lax.rsqrt(jnp.mean(wide_x * wide_x, -1, keepdims=True) + 1e-6)
        return wide_x * scale, scale

    def total_rows(k, h):
        def some(r, _):
            at = _at(k * sub + r * step, step)
            whole = _at(h * half + k * sub + r * step, step)
            da = (own_s[whole, :] + last_s[0, h, at, :].astype(F32) + last_s[1, h, at, :].astype(F32)).astype(LOW)
            last_s[0, h, at, :] = da
            both = da.astype(F32) * normal(whole)[0]
            sum_s[...] += sum(both[i:i + 8] for i in range(0, step, 8))

        lax.fori_loop(0, sub // step, some, None)

    def x_rows(k, h):
        def some(r, _):
            at = _at(k * sub + r * step, step)
            hat, scale = normal(_at(h * half + k * sub + r * step, step))
            d_hat = last_s[0, h, at, :].astype(F32) * gain
            inner = jnp.mean(d_hat * hat, -1, keepdims=True)
            ring_s[h, at, :] = ((d_hat - hat * inner) * scale + ring_s[h, at, :].astype(F32)).astype(LOW)

        lax.fori_loop(0, sub // step, some, None)
        save = pltpu.make_async_copy(ring_s.at[h, parts[k]], dx_ref.at[pl.ds(h * half + k * sub, sub)], sem_out.at[4 + 2 * k + h])
        save.start()
        return save

    def swap(k, dev, owner):
        line = gain_s.at[owner]
        return pltpu.make_async_remote_copy(src_ref=line, dst_ref=line, send_sem=gsend.at[k - 1], recv_sem=grecv.at[k - 1], device_id={"tp": dev}, device_id_type=MESH)

    saves = []
    for k in range(SUBS):
        for h in range(2):
            ring_c[h][k].wait_recv()
            total_rows(k, h)
        if k == SUBS - 1:
            gain_s[me] = sum_s[...].sum(axis=0, keepdims=True)
            for i in range(1, n):
                swap(i, lax.rem(me + i, n), me).start()
        saves += [x_rows(k, h) for h in range(2)]
    for k in range(1, n):
        swap(k, other, lax.rem(me + n - k, n)).wait_recv()
    by_gain_ref[...] = sum(gain_s[k] for k in range(n))
    for k in range(1, n):
        swap(k, lax.rem(me + k, n), me).wait_send()
    for one in [*ring_a, *ring_b, *ring_c[0], *ring_c[1]]:
        one.wait_send()
    for save in saves:
        save.wait()


def _results(*refs):
    k = len(refs) // 3
    sources, targets, rooms = refs[:k], refs[k:2 * k], refs[2 * k:3 * k]
    into, out = refs[-2:]
    pulls = [pltpu.make_async_copy(a, b, into.at[i]) for i, (a, b) in enumerate(zip(sources, rooms))]
    puts = [pltpu.make_async_copy(a, b, out.at[i]) for i, (a, b) in enumerate(zip(rooms, targets))]
    for pull in pulls:
        pull.start()
    for pull, put in zip(pulls, puts):
        pull.wait()
        put.start()
    for put in puts:
        put.wait()


def solution(mesh):
    n = mesh.shape["tp"]

    def step(x, dy, gain, wq, wk, wv, wo):
        tok, dim = x.shape
        heads = wq.shape[1] // HEAD
        hw = heads * HEAD
        width = hw + 2 * HEAD
        rows, cols, half = n * tok, heads * tok, tok // 2
        freq = np.float64(THETA) ** (-np.arange(HEAD // 2) / (HEAD // 2))

        def table(places):
            angle = np.asarray(places, np.float64)[:, None] * freq
            cos, sin = np.cos(angle), np.sin(angle)
            return jnp.asarray(np.stack([np.concatenate([cos, cos], 1), np.concatenate([-sin, sin], 1)]), F32)

        near, far = table(np.arange(tok)), table(np.arange(n) * tok)
        anywhere, vmem = pl.BlockSpec(memory_space=pl.ANY), pl.BlockSpec(memory_space=pltpu.VMEM)
        dma, scratch, shape = pltpu.SemaphoreType.DMA, pltpu.VMEM, jax.ShapeDtypeStruct
        size = hw
        most = max(rows, dim)
        ring = 16 + 2 * SUBS
        sends = 16 * UNITS
        _, _, *results = pl.pallas_call(
            functools.partial(_kernel, n, heads),
            out_shape=[shape((rows, dim), LOW), shape((rows, dim), LOW), shape((tok, dim), LOW), shape((1, dim), F32),
                       shape(wq.shape, LOW), shape(wk.shape, LOW), shape(wv.shape, LOW), shape(wo.shape, LOW)],
            in_specs=[anywhere, anywhere, vmem, anywhere, anywhere, anywhere, anywhere, vmem, vmem],
            out_specs=[anywhere, anywhere, anywhere, vmem, anywhere, anywhere, anywhere, anywhere],
            scratch_shapes=[
                scratch((2, tok, dim), LOW), scratch((width, dim), LOW), scratch((most, hw), LOW),
                scratch((n, cols, HEAD), LOW), scratch((most, HEAD), LOW), scratch((HEAD, rows), LOW), scratch((most, HEAD), LOW), scratch((HEAD + 8, rows), LOW),
                scratch((1, cols), F32), scratch((2, cols, HEAD), LOW), scratch((cols // UNITS, HEAD), LOW), scratch((1, cols), F32), scratch((n, 1, cols), F32), scratch((n, HEAD + 8, cols), F32),
                scratch((HEAD, cols), F32), scratch((rows, HEAD), F32), scratch((rows, HEAD), F32), scratch((rows, width), LOW), scratch((width + hw, rows), LOW),
                scratch((4, tok, dim), LOW), scratch((2, half, dim), LOW), scratch((2, 2, half, dim), LOW), scratch((tok, dim), F32),
                scratch((most, size), LOW), scratch((n, 1, dim), F32), scratch((8, dim), F32),
                dma((2, sends)), dma((2, sends)), dma((ring,)), dma((ring,)), dma((n - 1,)), dma((n - 1,)), dma((5,)), dma((dim // hw,)), dma((2, UNITS)), dma((2,)), dma((4 + 2 * SUBS,))],
            compiler_params=pltpu.CompilerParams(collective_id=0, has_side_effects=True, vmem_limit_bytes=VMEM),
            name="layer",
        )(x, dy, gain, wq, wk, wv, wo, near, far)
        kept = [results[i] for i in (2, 3, 4, 0, 5, 1)]
        out = pl.pallas_call(
            _results,
            out_shape=[shape(t.shape, t.dtype) for t in kept],
            in_specs=[anywhere] * len(kept),
            out_specs=[anywhere] * len(kept),
            scratch_shapes=[*[scratch(t.shape, t.dtype) for t in kept], dma((len(kept),)), dma((len(kept),))],
            compiler_params=pltpu.CompilerParams(vmem_limit_bytes=VMEM),
            name="results",
        )(*kept)
        return out[3], out[5], out[0], out[1], out[2], out[4]

    tokens, columns = P(("dp", "tp"), None), P(None, "tp")
    return jax.shard_map(
        step,
        mesh=mesh,
        in_specs=(tokens, tokens, P(None), columns, columns, columns, P("tp", None)),
        out_specs=(tokens, P("dp", None), P("dp", "tp"), P("dp", "tp"), P("dp", "tp"), P(("dp", "tp"), None)),
        check_vma=False,
    )
```

```python
import functools

import jax
import jax.numpy as jnp
import numpy as np
from jax import lax
from jax.experimental import pallas as pl
from jax.experimental.pallas import tpu as pltpu
from jax.sharding import PartitionSpec as P

HEAD = 128
THETA = 10000
NEG = -1e30
HIDDEN = 2 * NEG
LOG2E = 1.4426950408889634
VMEM = 67_043_328
MESH = pl.DeviceIdType.MESH
F32, LOW = jnp.float32, jnp.bfloat16
UNITS = 3
SUBS = 6


def _dot(a, b, ca, cb):
    return lax.dot_general(a, b, (((ca,), (cb,)), ((), ())), preferred_element_type=F32)


def _at(start, size, unit=None):
    return pl.ds(pl.multiple_of(start, unit or size), size)


def _kernel(n, heads, x_ref, dy_ref, gain_ref, wq_ref, wk_ref, wv_ref, wo_ref, near_hbm, far_hbm,
            a_ref, g_ref, dx_ref, by_gain_ref, by_wq_ref, by_wk_ref, by_wv_ref, by_wo_ref,
            near_ref, far_ref, chunk_s, wt_s, wo_s, q_s, k_s, kt_s, v_s, vt_s, lse_s, do_s, do_u, delta_s, top_s, mix_s, dq_s, dk_s, dv_s, grads_s, turn_s,
            pair_s, ring_s, last_s, own_s, flow_s, gain_s, sum_s, send, recv, rsend, rrecv, gsend, grecv, loc, sem_wo, sem_load, sem_in, sem_out):
    tok, dim = x_ref.shape
    half, quarter, hw = tok // 2, tok // 4, heads * HEAD
    unit = tok // UNITS
    width = hw + 2 * HEAD
    chips = n // 2
    me = lax.axis_index("tp")
    chip, core = me // 2, lax.rem(me, 2)
    other = chip * 2 + 1 - core
    lchip, rchip, ochip = lax.rem(chip + chips - 1, chips), lax.rem(chip + 1, chips), lax.rem(chip + chips // 2, chips)
    left, right, across = lchip * 2 + core, rchip * 2 + core, ochip * 2 + core
    e = HEAD**-0.5 * LOG2E

    few = unit // 4

    def part(c):
        return unit // 2 * c

    away = 1 - core
    pieces = {}

    def piece(name, sent, got, to, size=2 * few):
        pieces[name] = (len(pieces) * UNITS, sent, got, to, size)

    for name, to, c_from in (("r", right, lchip), ("l", left, rchip)):
        for k in range(2):
            piece(name + str(k), (chip, k, part(core)), (c_from, k, part(core)), to)
    piece("p", (chip, core, part(away)), (chip, away, part(core)), other)
    piece("q", (chip, core, part(core)), (chip, away, part(away)), other)
    for name, c in (("pl", lchip), ("pr", rchip), ("po", ochip)):
        for k in range(2):
            piece(name + str(k), (c, k, part(core)), (c, k, part(away)), other)
    full_pieces = len(pieces)
    for name, to, c_over, shift in (("r", right, lchip, 0), ("l", left, rchip, few)):
        for k in range(2):
            piece(name + str(k + 2), (c_over, k, part(core) + shift), (ochip, k, part(core) + shift), to, few)

    def each(do):
        lax.fori_loop(0, UNITS, lambda k, _: do(k), None)

    def rows(dev):
        return _at(dev * tok, tok)

    def copy(z, name, k, sending=True):
        i, sent, got, to, size = pieces[name]
        c, e_, first = sent if sending else got
        at = first + unit * k
        full = (a_ref, g_ref)[z].at[_at((c * 2 + e_) * tok + at, size, few)]
        own = name in ("p", "q")
        return pltpu.make_async_remote_copy(src_ref=chunk_s.at[z, _at(at, size, few)] if own else full, dst_ref=full,
                                            send_sem=send.at[z, i + k], recv_sem=recv.at[z, i + k], device_id={"tp": to}, device_id_type=MESH)

    def start(z, k, *names):
        for name in names:
            copy(z, name, k).start()

    def arrived(z, k, *names):
        for name in names:
            copy(z, name, k, False).wait_recv()

    def order(s):
        t = s // 2
        middle, final = (t + 1) // 2 - 2 * (t // 3), t // 3
        c = lax.rem(chip + middle * (chips - 1 - (chips - 2) * lax.rem(s, 2)) + final * (chips // 2), chips)
        k = (1 - middle - final) * lax.rem(core + s, 2) + middle * (t - 1) + final * lax.rem(s, 2)
        return c * 2 + k

    def load(z, s, k):
        dev, slot = order(s), lax.rem(s, 2)
        return pltpu.make_async_copy((a_ref, g_ref)[z].at[_at(dev * tok + k * unit, unit)], chunk_s.at[slot, _at(k * unit, unit)], sem_load.at[slot, k])

    def pass_on(z, s):
        for e_ in range(2):

            @pl.when(s == 2 + 2 * e_)
            def _(e_=str(e_), over=str(e_ + 2)):
                def one(k):
                    arrived(z, k, "r" + e_, "l" + e_)
                    start(z, k, "r" + over, "l" + over, "pl" + e_, "pr" + e_)

                def rest(k):
                    arrived(z, k, "pl" + e_)
                    load(z, s, k).start()

                def both(k):
                    one(k)
                    rest(k)

                if z == 1:
                    each(one)
                    return

                lax.fori_loop(0, UNITS - 1, lambda k, _: both(k), None)
                one(UNITS - 1)
                if z == 0 and e_ == "1":
                    each(lambda k: start(1, k, "r0", "l0"))
                    each(lambda k: start(1, k, "r1", "l1"))
                rest(UNITS - 1)

            @pl.when(s == 6 + e_)
            def _(e_=str(e_), over=str(e_ + 2)):
                def one(k):
                    arrived(z, k, "r" + over, "l" + over)
                    start(z, k, "po" + e_)

                each(one)

    def fetch_next(z, s):
        for step, name in ((3, "pr0"), (5, "pr1"), (6, "po0"), (7, "po1")):

            @pl.when(s == step)
            def _(name=name):
                each(lambda k: arrived(z, k, name))

        if z == 1:

            @pl.when(s == 2)
            def _():
                each(lambda k: arrived(z, k, "pl0"))

            @pl.when(s == 4)
            def _():
                each(lambda k: arrived(z, k, "pl1"))

            each(lambda k: load(z, s, k).start())
            return

        @pl.when((s < n) & (s != 2) & (s != 4))
        def _():
            each(lambda k: load(z, s, k).start())

    loads_x = [pltpu.make_async_copy(x_ref.at[pl.ds(k * unit, unit)], chunk_s.at[0, pl.ds(k * unit, unit)], sem_load.at[0, k]) for k in range(UNITS)]
    for one in loads_x:
        one.start()
    load_dy = pltpu.make_async_copy(dy_ref, chunk_s.at[1], loc.at[1])
    load_dy.start()
    loads = [pltpu.make_async_copy(wq_ref, flow_s, loc.at[2]), pltpu.make_async_copy(wk_ref, k_s, loc.at[3]), pltpu.make_async_copy(wv_ref, v_s, loc.at[4])]
    for one in loads:
        one.start()
    loads += [pltpu.make_async_copy(wo_ref.at[:, pl.ds(i * hw, hw)], wo_s.at[pl.ds(i * hw, hw)], sem_wo.at[i]) for i in range(dim // hw)]
    loads += [pltpu.make_async_copy(near_hbm, near_ref, loc.at[5]), pltpu.make_async_copy(far_hbm, far_ref, loc.at[6])]
    for one in loads[3:]:
        one.start()
    barrier = pltpu.get_barrier_semaphore()
    for k in range(1, n):
        pl.semaphore_signal(barrier, inc=1, device_id={"tp": lax.rem(me + k, n)}, device_id_type=MESH)

    gain = gain_ref[...].reshape(1, dim).astype(F32)
    block = 32

    def norm(r, _):
        at = _at(r * block, block)
        wide = chunk_s[0, at, :].astype(F32)
        scale = lax.rsqrt(jnp.mean(wide * wide, -1, keepdims=True) + 1e-6)
        chunk_s[0, at, :] = (wide * scale * gain).astype(LOW)

    for k, one in enumerate(loads_x):
        one.wait()
        lax.fori_loop(k * unit // block, (k + 1) * unit // block, norm, None)
        if k == 0:
            pl.semaphore_wait(barrier, n - 1)
        start(0, k, "p")
    each(lambda k: start(0, k, "q"))
    keep = pltpu.make_async_copy(chunk_s.at[0], a_ref.at[rows(me)], loc.at[0])
    keep.start()
    load_dy.wait()
    keep_dy = pltpu.make_async_copy(chunk_s.at[1], g_ref.at[rows(me)], loc.at[1])
    keep_dy.start()
    keep.wait()
    each(lambda k: arrived(0, k, "p"))
    each(lambda k: start(0, k, "r0", "l0"))
    each(lambda k: start(0, k, "r1", "l1"))
    each(lambda k: start(1, k, "p", "q"))
    keep_dy.wait()
    for one in loads:
        one.wait()

    def lay_weights(i, _):
        at = _at(i * tok, tok)
        wt_s[:hw, at] = flow_s[at, :].T
        wt_s[hw:hw + HEAD, at] = k_s[at, :].T
        wt_s[hw + HEAD:, at] = v_s[at, :].T

    def lay_wo(i, _):
        at = _at(i * hw, hw)
        wo_s[at, :] = wo_s[at, :].T

    lax.fori_loop(0, dim // tok, lay_weights, None)
    lax.fori_loop(0, dim // hw, lay_wo, None)
    each(lambda k: arrived(0, k, "q"))
    each(lambda k: arrived(1, k, "p", "q"))
    for z in range(2):
        each(lambda k, z=z: [copy(z, name, k).wait_send() for name in ("p", "q")] and None)

    cols = heads * tok
    side_by = heads * unit
    groups = [pl.ds(k * side_by, side_by) for k in range(UNITS)]

    def spot(h, k):
        return pl.ds(k * side_by + h * unit, unit)

    lanes = [pl.ds(h * HEAD, HEAD) for h in range(heads)]

    def tables(j, at=slice(None)):
        ca, sa = near_ref[0, at, :], near_ref[1, at, :]
        cb, sb = far_ref[0, pl.ds(j, 1), :], far_ref[1, pl.ds(j, 1), :]
        return ca * cb - sa * sb, sa * cb + ca * sb

    def turned(t, cos, sin):
        return (t * cos + pltpu.roll(t, HEAD // 2, 1) * sin).astype(LOW)

    def project(j, slot):
        y = _dot(chunk_s[slot], wt_s[...], 1, 1).astype(LOW).astype(F32)
        cos, sin = tables(j)
        at = rows(j)
        for h in range(heads):
            q = turned(y[:, h * HEAD:(h + 1) * HEAD], cos, sin)
            for k in range(UNITS):
                q_s[j, spot(h, k), :] = q[k * unit:(k + 1) * unit]
        k = turned(y[:, hw:hw + HEAD], cos, sin)
        v = y[:, hw + HEAD:].astype(LOW)
        k_s[at, :] = k
        kt_s[:, at] = k.T
        v_s[at, :] = v
        vt_s[:HEAD, at] = v.T

    def visible(k, more=0):
        shape = ((k + 1) * unit + more, side_by)
        return lax.rem(lax.broadcasted_iota(jnp.int32, shape, 1), unit) + k * unit >= lax.broadcasted_iota(jnp.int32, shape, 0)

    def blocks_of(j, i, masked):
        return [(k, at, pl.ds(pl.multiple_of(i * tok, tok), (k + 1) * unit if masked else tok)) for k, at in enumerate(groups)]

    def seen_block(j, i, masked):
        parts_of = blocks_of(j, i, masked)
        if masked:
            scores = [_dot(k_s[here, :], q_s[j, at, :], 1, 1) for _, at, here in parts_of]
        else:
            wide = _dot(k_s[parts_of[0][2], :], q_s[j], 1, 1)
            scores = [wide[:, k * side_by:(k + 1) * side_by] for k in range(UNITS)]
        weights, keeps = [], []
        for (k, at, _), s in zip(parts_of, scores):
            if masked:
                s = jnp.where(visible(k), s, HIDDEN)
            old = top_s[j, :, at]
            top = jnp.maximum(old, s.max(axis=0, keepdims=True))
            top_s[j, :, at] = top
            weights.append(jnp.exp2((s - top) * e).astype(LOW))
            keeps.append(jnp.exp2((old - top) * e))
        for (_, at, here), p, kept in zip(parts_of, weights, keeps):
            mix_s[j, :, at] = mix_s[j, :, at] * kept + _dot(vt_s[:, here], p, 1, 0)

    vt_s[HEAD:, :] = jnp.ones((8, n * tok), LOW)

    def clear(j, _):
        top_s[j] = jnp.full((1, cols), NEG, F32)
        mix_s[j] = jnp.zeros((HEAD + 8, cols), F32)

    lax.fori_loop(0, n, clear, None)
    dk_s[...] = jnp.zeros_like(dk_s)
    dv_s[...] = jnp.zeros_like(dv_s)

    def keep_d_out(slot):
        d_out = _dot(chunk_s[slot], wo_s[...], 1, 0).astype(LOW)
        for h in range(heads):
            for k in range(UNITS):
                do_s[slot, spot(h, k), :] = d_out[k * unit:(k + 1) * unit, h * HEAD:(h + 1) * HEAD]

    def x_step(s, _):
        j = order(s)
        early = (lax.rem(s, 2) == 0) & (s < 6)
        middle = (s == 5) | (s == 6)

        @pl.when(s > 0)
        def _():
            each(lambda k: load(0, s, k).wait())

        @pl.when(early)
        def _():
            fetch_next(0, s + 1)

        project(j, lax.rem(s, 2))

        seen_block(j, j, True)

        def earlier(t, _):
            @pl.when(middle & (t == 2 * (s - 5)))
            def _():
                pass_on(0, s + 1)

            @pl.when(middle & (t == 2 * (s - 4)))
            def _():
                fetch_next(0, s + 1)

            i = order(t)
            seen_block(jnp.maximum(i, j), jnp.minimum(i, j), False)

        lax.fori_loop(0, s, earlier, None)

        @pl.when(s == 1)
        def _():
            for t in range(2):
                each(lambda k, t=t: load(1, t, k).start())

            def one(t, _):
                each(lambda k: load(1, t, k).wait())
                keep_d_out(t)

            lax.fori_loop(0, 2, one, None)

        @pl.when((s == 1) | (s == 3))
        def _():
            pass_on(0, s + 1)
            fetch_next(0, s + 1)

    lax.fori_loop(0, n, x_step, None)


    steps = 4 * UNITS
    wraps = rchip > ochip
    turns = ochip == chips - 1
    pause = jnp.where(turns, steps - 1, steps - UNITS)

    def unit_order(t):
        u = jnp.where(turns, t + 1, t)
        g = u // UNITS
        first = turns & (t < 2 * UNITS - 1)
        last = turns & (t == steps - 1)
        side = jnp.where(first, lax.rem(t, 2), jnp.where(last, 1, jnp.where(turns, 2, jnp.where(g == 0, 0, jnp.where(g == 3, 1, 2)))))
        e_ = jnp.where(side == 2, jnp.where(turns, g - 2, g - 1), 1)
        return side, e_, jnp.where(first, t // 2, jnp.where(last, UNITS - 1, lax.rem(u, UNITS)))

    def unit_dev(side, e_):
        return jnp.where(side == 0, lchip, jnp.where(side == 1, rchip, ochip)) * 2 + e_

    def unit_pass_on(t):
        side, which, k = unit_order(t)

        @pl.when(side == 0)
        def _():
            arrived(1, k, "r1", "l1")
            start(1, k, "r3", "l3", "pl1", "pr1")

        for e_ in range(2):

            @pl.when((side == 2) & (which == e_))
            def _(e_=str(e_), over=str(e_ + 2)):
                arrived(1, k, "r" + over, "l" + over)
                start(1, k, "po" + e_)

    def unit_load(t):
        side, e_, k = unit_order(t)
        slot = lax.rem(t, 2)
        return pltpu.make_async_copy(g_ref.at[_at(unit_dev(side, e_) * tok + k * unit, unit)], chunk_s.at[0, _at(slot * unit, unit)], sem_load.at[slot, 0])

    def unit_fetch(t):
        side, which, k = unit_order(t)
        for name, test in (("pl1", side == 0), ("pr1", side == 1), ("po0", (side == 2) & (which == 0)), ("po1", (side == 2) & (which == 1))):

            @pl.when(test)
            def _(name=name):
                arrived(1, k, name)

        unit_load(t).start()

    def backward(s):
        j = order(s)
        slot = lax.rem(s, 2)

        @pl.when(s >= 2)
        def _():
            each(lambda k: load(1, s, k).wait())

        @pl.when((s == 2) | (s == 4))
        def _():
            fetch_next(1, s + 1)

        @pl.when(s == 6)
        def _():
            pass_on(1, s + 1)

        @pl.when(s >= 2)
        def _():
            keep_d_out(slot)

        total = mix_s[j, HEAD:HEAD + 1, :]
        lse_s[...] = top_s[j] * e + jnp.log2(total)
        for h in range(heads):
            for k in range(UNITS):
                at = spot(h, k)
                out = (mix_s[j, :HEAD, at] * (1 / total[:, k * side_by + h * unit:k * side_by + (h + 1) * unit])).astype(LOW)
                turn_s[pl.ds(width + h * HEAD, HEAD), _at(j * tok + k * unit, unit)] = out
                delta_s[:, at] = (do_s[slot, at, :].astype(F32).T * out.astype(F32)).sum(axis=0, keepdims=True)
        dq_s[...] = jnp.zeros_like(dq_s)

        def block(i):
            here = rows(i)
            scores = _dot(k_s[here, :], q_s[j], 1, 1)
            dps = _dot(v_s[here, :], do_s[slot], 1, 1)
            ps, dss = [], []
            for k, at in enumerate(groups):
                p = jnp.exp2(scores[:, k * side_by:(k + 1) * side_by] * e - lse_s[:, at])
                dss.append((p * (dps[:, k * side_by:(k + 1) * side_by] - delta_s[:, at])).astype(LOW))
                ps.append(p.astype(LOW))
            p, ds = jnp.concatenate(ps, axis=1), jnp.concatenate(dss, axis=1)
            dv_s[here, :] += _dot(p, do_s[slot], 1, 0)
            dk_s[here, :] += _dot(ds, q_s[j], 1, 0)
            dq_s[...] += _dot(kt_s[:, here], ds, 1, 0)

        def own_block():
            parts_of = blocks_of(j, j, True)
            scores = [_dot(k_s[here, :], q_s[j, at, :], 1, 1) for _, at, here in parts_of]
            dps = [_dot(v_s[here, :], do_s[slot, at, :], 1, 1) for _, at, here in parts_of]
            for (k, at, here), sc, dp in zip(parts_of, scores, dps):
                p = jnp.where(visible(k), jnp.exp2(sc * e - lse_s[:, at]), 0.0)
                ds = (p * (dp - delta_s[:, at])).astype(LOW)
                dv_s[here, :] += _dot(p.astype(LOW), do_s[slot, at, :], 1, 0)
                dk_s[here, :] += _dot(ds, q_s[j, at, :], 1, 0)
                dq_s[:, at] += _dot(kt_s[:, here], ds, 1, 0)

        ahead = jnp.maximum(j - 3, 0)

        def one_block(i, _):
            @pl.when((s == 5) & (i == ahead))
            def _():
                pass_on(1, s + 1)

            block(i)

        lax.fori_loop(0, j, one_block, None)

        units_next = (s == 3) & jnp.logical_not(wraps)
        whole_next = (s == 1) | ((s == 3) & wraps)
        here_next = (s == 5) | (s == 6)

        @pl.when(whole_next)
        def _():
            pass_on(1, s + 1)

        @pl.when(units_next)
        def _():
            unit_pass_on(0)

        @pl.when(here_next)
        def _():
            fetch_next(1, s + 1)

        own_block()

        @pl.when(whole_next)
        def _():
            fetch_next(1, s + 1)

        @pl.when(units_next)
        def _():
            unit_fetch(0)

        cos, sin = tables(j)
        for h in range(heads):
            whole_dq = jnp.concatenate([dq_s[:, spot(h, k)] for k in range(UNITS)], axis=1)
            one = (whole_dq * HEAD**-0.5).T.astype(LOW).astype(F32)
            grads_s[rows(j), lanes[h]] = turned(one, cos, -sin)


    def unit_backward(t):
        side, e_, k = unit_order(t)
        j, slot = unit_dev(side, e_), lax.rem(t, 2)
        unit_load(t).wait()

        d_out = _dot(chunk_s[0, _at(slot * unit, unit), :], wo_s[...], 1, 0).astype(LOW)
        at = _at(j * tok + k * unit, unit)
        mine = [pl.ds(h * unit, unit) for h in range(heads)]
        for h in range(heads):
            lane = _at(k * side_by + h * unit, unit)
            total = mix_s[j, HEAD:HEAD + 1, lane]
            out = (mix_s[j, :HEAD, lane] * (1 / total)).astype(LOW)
            turn_s[pl.ds(width + h * HEAD, HEAD), at] = out
            one = d_out[:, h * HEAD:(h + 1) * HEAD]
            do_u[mine[h], :] = one
            delta_s[:, mine[h]] = (one.astype(F32).T * out.astype(F32)).sum(axis=0, keepdims=True)
            lse_s[:, mine[h]] = top_s[j, :, lane] * e + jnp.log2(total)
        across_u = side_by
        q_u = q_s.at[j, _at(k * side_by, side_by)]
        dq_s[:, :across_u] = jnp.zeros((HEAD, across_u), F32)

        def span(first, count, masked):
            here = _at(first * tok, count * tok, tok)
            scores = _dot(k_s[here, :], q_u[...], 1, 1)
            dps = _dot(v_s[here, :], do_u[...], 1, 1)
            ps, dss = [], []
            for b in range(count):
                p = jnp.exp2(scores[b * tok:(b + 1) * tok] * e - lse_s[:, :across_u])
                if masked and b == count - 1:
                    query = lax.rem(lax.broadcasted_iota(jnp.int32, (tok, across_u), 1), unit) + k * unit
                    p = jnp.where(query >= lax.broadcasted_iota(jnp.int32, (tok, across_u), 0), p, 0.0)
                dss.append((p * (dps[b * tok:(b + 1) * tok] - delta_s[:, :across_u])).astype(LOW))
                ps.append(p.astype(LOW))
            p, ds = jnp.concatenate(ps, axis=0), jnp.concatenate(dss, axis=0)
            dv_s[here, :] += _dot(p, do_u[...], 1, 0)
            dk_s[here, :] += _dot(ds, q_u[...], 1, 0)
            dq_s[:, :across_u] += _dot(kt_s[:, here], ds, 1, 0)

        most = 3
        times = j // most

        @pl.when(t + 1 < steps)
        def _():
            unit_pass_on(t + 1)

        lax.fori_loop(0, times, lambda i, _: span(i * most, most, False), None)

        @pl.when(t + 1 < steps)
        def _():
            unit_fetch(t + 1)

        for rest in range(most):

            @pl.when(j - times * most == rest)
            def _(rest=rest):
                span(j - rest, rest + 1, True)

        cos, sin = tables(j, _at(k * unit, unit))
        for h in range(heads):
            one = (dq_s[:, mine[h]] * HEAD**-0.5).T.astype(LOW).astype(F32)
            grads_s[at, lanes[h]] = turned(one, cos, -sin)

    def finish(j, _):
        cos, sin = tables(j)
        at = rows(j)
        one = (dk_s[at, :] * HEAD**-0.5).astype(LOW).astype(F32)
        grads_s[at, hw:hw + HEAD] = turned(one, cos, -sin)
        grads_s[at, hw + HEAD:] = dv_s[at, :].astype(LOW)

    wide = dim // 2

    def term(dst, dev, first, size, *adds, only=None):
        at = _at(dev * tok + first, size)

        def column(c, _):
            here = _at(c * wide, wide)
            t = _dot(grads_s[at, :], wt_s[:, here], 1, 0)
            for add in adds:
                t = t + add[:, here].astype(F32)
            dst[:, here] = t.astype(dst.dtype)

        if only is None:
            lax.fori_loop(0, dim // wide, column, None)
        else:
            column(only, None)

    there = [ochip, rchip, lchip, chip]
    plan = [(0, 0, half), (0, half, half), (0, 0, half), (0, half, half),
            (1, half, half), (2, 0, half), (1, 0, half), (2, half, half), (3, 0, half), (3, half, half)]

    def remote(i, src, dst, dev):
        return pltpu.make_async_remote_copy(src_ref=src, dst_ref=dst, send_sem=rsend.at[i], recv_sem=rrecv.at[i], device_id={"tp": dev}, device_id_type=MESH)

    def columns_of(i):
        return (pl.ds(i // 2 * wide, wide),) if i < 4 else ()

    def span_of(i):
        place, first, size = plan[i]
        return pair_s.at[(place, pl.ds(first, size), *columns_of(i))]

    def out(i):
        return chunk_s.at[(1, pl.ds(i % 2 * half, half), *columns_of(i))] if i < 4 else chunk_s.at[i % 4 // 2, pl.ds(i % 2 * half, half)]

    def pair(i):
        return remote(i, out(i), span_of(i), other)

    base = len(plan)
    sub = half // SUBS
    ring_a = [remote(base + i, span_of(i), ring_s.at[(i % 2, slice(None), *columns_of(i))], (right, left)[i % 2]) for i in range(4)]
    ring_b = [remote(base + 4, span_of(4), last_s.at[0, 1], right), remote(base + 5, span_of(5), last_s.at[1, 0], left)]

    def ring_c(h, k):
        at = _at(k * sub, sub)
        src = pair_s.at[1, at] if h == 0 else pair_s.at[2, _at(half + k * sub, sub)]
        return remote(base + 6 + h * SUBS + k, src, last_s.at[h, h, at], (right, left)[h])

    def every_sub(do):
        lax.fori_loop(0, SUBS, lambda k, _: do(k), None)

    def give(i):
        place, first, size = plan[i]
        if i >= 8:
            pair(i - 4).wait_send()
        target = chunk_s.at[1, pl.ds(i % 2 * half, half)] if i < 4 else out(i)
        term(target, there[place] * 2 + 1 - core, first, size, only=i // 2 if i < 4 else None)
        pair(i).start()

    def take(i, *adds):
        place, first, size = plan[i]
        pair(i).wait_recv()
        slot = pair_s.at[place, pl.ds(first, size)]
        term(slot, there[place] * 2 + core, first, size, slot, *adds, only=i // 2 if i < 4 else None)

    def first_terms():
        lax.fori_loop(0, 2, lambda i, _: finish(ochip * 2 + i, _), None)
        give(0)
        give(1)
        for i in range(4):
            take(i)
            ring_a[i].start()
            if i < 2:
                give(i + 2)

    whole = jnp.where(wraps, n, 4)
    break_at = jnp.where(wraps, n, 4 + pause)

    def g_step(t, _):
        @pl.when(t < whole)
        def _():
            backward(t)

        @pl.when(t == break_at)
        def _():
            first_terms()

        @pl.when((t >= whole) & (t != break_at))
        def _():
            unit_backward(t - whole - (t > break_at).astype(jnp.int32))

    lax.fori_loop(0, jnp.where(wraps, n, 4 + steps) + 1, g_step, None)
    lax.fori_loop(2, n, lambda i, _: finish(lax.rem(ochip * 2 + i, n), _), None)
    for i in range(4):
        pair(i).wait_send()
    give(4)
    give(5)
    for i in (4, 5):
        take(i)
        ring_b[i - 4].start()
    for i in range(6, 10):
        give(i)

    def lay(j, _):
        turn_s[:width, rows(j)] = grads_s[rows(j), :].T

    lax.fori_loop(0, n, lay, None)
    for i in (8, 9):
        place, first, size = plan[i]
        pair(i).wait_recv()
        term(own_s.at[pl.ds(first, size)], me, first, size, span_of(i))

    for i in range(6, 10):
        pair(i).wait_send()
    size = hw
    dw_s, dwo_s = chunk_s.at[0, pl.ds(0, size), pl.ds(0, width)], chunk_s.at[1, pl.ds(0, hw), pl.ds(0, size)]
    blocks = dim // size
    flows = [wo_s, flow_s]

    def fetch(s, kind):
        return pltpu.make_async_copy((a_ref, g_ref)[kind].at[:, _at(s * size, size)], flows[kind], sem_in.at[kind])

    def puts(s):
        at = _at(s * size, size)
        return [pltpu.make_async_copy(dw_s.at[:, :hw], by_wq_ref.at[at], sem_out.at[0]),
                pltpu.make_async_copy(dw_s.at[:, hw:hw + HEAD], by_wk_ref.at[at], sem_out.at[1]),
                pltpu.make_async_copy(dw_s.at[:, hw + HEAD:], by_wv_ref.at[at], sem_out.at[2])]

    def put_o(s):
        return pltpu.make_async_copy(dwo_s, by_wo_ref.at[:, _at(s * size, size)], sem_out.at[3])

    fetch(0, 0).start()
    fetch(0, 1).start()

    def weights(s, _):
        fetch(s, 0).wait()
        dw = _dot(turn_s[:width, :], flows[0][...], 1, 0)

        @pl.when(s + 1 < blocks)
        def _():
            fetch(s + 1, 0).start()

        @pl.when(s > 0)
        def _():
            for put in puts(s - 1):
                put.wait()

        dw_s[...] = dw.T.astype(LOW)
        for put in puts(s):
            put.start()
        fetch(s, 1).wait()
        dwo = _dot(turn_s[width:, :], flows[1][...], 1, 0)

        @pl.when(s + 1 < blocks)
        def _():
            fetch(s + 1, 1).start()

        @pl.when(s > 0)
        def _():
            put_o(s - 1).wait()

        dwo_s[...] = dwo.astype(LOW)
        put_o(s).start()

    lax.fori_loop(0, blocks // 2, weights, None)
    for h in range(2):
        for one in ring_a[h::2]:
            one.wait_recv()
        take(6 + h, ring_s.at[h])
        every_sub(lambda k, h=h: ring_c(h, k).start())
    for z in range(2):
        def sent_full(i, _, z=z):
            first = a_ref.at[pl.ds(0, 2 * few)]
            pltpu.make_async_remote_copy(src_ref=first, dst_ref=first, send_sem=send.at[z, i], recv_sem=recv.at[z, i], device_id={"tp": other}, device_id_type=MESH).wait_send()

        def sent_few(i, _, z=z):
            first = a_ref.at[pl.ds(0, few)]
            pltpu.make_async_remote_copy(src_ref=first, dst_ref=first, send_sem=send.at[z, i], recv_sem=recv.at[z, i], device_id={"tp": other}, device_id_type=MESH).wait_send()

        lax.fori_loop(0, 4 * UNITS, sent_full, None)
        lax.fori_loop(6 * UNITS, full_pieces * UNITS, sent_full, None)
        lax.fori_loop(full_pieces * UNITS, len(pieces) * UNITS, sent_few, None)
    lax.fori_loop(blocks // 2, blocks, weights, None)
    for put in puts(blocks - 1):
        put.wait()
    put_o(blocks - 1).wait()

    pulls = [pltpu.make_async_copy(x_ref.at[pl.ds(h * half, half)], pair_s.at[3, pl.ds(h * half, half)], loc.at[h]) for h in range(2)]
    pulls += [pltpu.make_async_copy(dy_ref.at[pl.ds(h * half, half)], ring_s.at[h], loc.at[2 + h]) for h in range(2)]
    for pull in pulls:
        pull.start()
    sum_s[...] = jnp.zeros_like(sum_s)
    for pull in pulls:
        pull.wait()
    for one in ring_b:
        one.wait_recv()
    step = 32

    def normal(at):
        wide_x = pair_s[3, at, :].astype(F32)
        scale = lax.rsqrt(jnp.mean(wide_x * wide_x, -1, keepdims=True) + 1e-6)
        return wide_x * scale, scale

    def total_rows(k, h):
        def some(r, _):
            at = _at(k * sub + r * step, step)
            whole = _at(h * half + k * sub + r * step, step)
            da = (own_s[whole, :] + last_s[0, h, at, :].astype(F32) + last_s[1, h, at, :].astype(F32)).astype(LOW)
            last_s[0, h, at, :] = da
            both = da.astype(F32) * normal(whole)[0]
            sum_s[...] += sum(both[i:i + 8] for i in range(0, step, 8))

        lax.fori_loop(0, sub // step, some, None)

    def save(k, h):
        return pltpu.make_async_copy(ring_s.at[h, _at(k * sub, sub)], dx_ref.at[_at(h * half + k * sub, sub)], sem_out.at[4 + 2 * k + h])

    def x_rows(k, h):
        def some(r, _):
            at = _at(k * sub + r * step, step)
            hat, scale = normal(_at(h * half + k * sub + r * step, step))
            d_hat = last_s[0, h, at, :].astype(F32) * gain
            inner = jnp.mean(d_hat * hat, -1, keepdims=True)
            ring_s[h, at, :] = ((d_hat - hat * inner) * scale + ring_s[h, at, :].astype(F32)).astype(LOW)

        lax.fori_loop(0, sub // step, some, None)
        save(k, h).start()

    def swap(k, dev, owner):
        line = gain_s.at[owner]
        return pltpu.make_async_remote_copy(src_ref=line, dst_ref=line, send_sem=gsend.at[k - 1], recv_sem=grecv.at[k - 1], device_id={"tp": dev}, device_id_type=MESH)

    def totals(k):
        for h in range(2):
            ring_c(h, k).wait_recv()
            total_rows(k, h)

    def results(k):
        for h in range(2):
            x_rows(k, h)

    def both_rows(k, _):
        totals(k)
        results(k)

    lax.fori_loop(0, SUBS - 1, both_rows, None)
    totals(SUBS - 1)
    gain_s[me] = sum_s[...].sum(axis=0, keepdims=True)
    for i in range(1, n):
        swap(i, lax.rem(me + i, n), me).start()
    results(SUBS - 1)
    for k in range(1, n):
        swap(k, other, lax.rem(me + n - k, n)).wait_recv()
    by_gain_ref[...] = sum(gain_s[k] for k in range(n))
    for k in range(1, n):
        swap(k, lax.rem(me + k, n), me).wait_send()
    for one in [*ring_a, *ring_b]:
        one.wait_send()

    def ended(k):
        for h in range(2):
            ring_c(h, k).wait_send()
            save(k, h).wait()

    every_sub(ended)


def _results(*refs):
    k = len(refs) // 3
    sources, targets, rooms = refs[:k], refs[k:2 * k], refs[2 * k:3 * k]
    into, out = refs[-2:]
    pulls = [pltpu.make_async_copy(a, b, into.at[i]) for i, (a, b) in enumerate(zip(sources, rooms))]
    puts = [pltpu.make_async_copy(a, b, out.at[i]) for i, (a, b) in enumerate(zip(rooms, targets))]
    for pull in pulls:
        pull.start()
    for pull, put in zip(pulls, puts):
        pull.wait()
        put.start()
    for put in puts:
        put.wait()


def solution(mesh):
    n = mesh.shape["tp"]

    def step(x, dy, gain, wq, wk, wv, wo):
        tok, dim = x.shape
        heads = wq.shape[1] // HEAD
        hw = heads * HEAD
        width = hw + 2 * HEAD
        rows, cols, half = n * tok, heads * tok, tok // 2
        freq = np.float64(THETA) ** (-np.arange(HEAD // 2) / (HEAD // 2))

        def table(places):
            angle = np.asarray(places, np.float64)[:, None] * freq
            cos, sin = np.cos(angle), np.sin(angle)
            return jnp.asarray(np.stack([np.concatenate([cos, cos], 1), np.concatenate([-sin, sin], 1)]), F32)

        near, far = table(np.arange(tok)), table(np.arange(n) * tok)
        anywhere, vmem = pl.BlockSpec(memory_space=pl.ANY), pl.BlockSpec(memory_space=pltpu.VMEM)
        dma, scratch, shape = pltpu.SemaphoreType.DMA, pltpu.VMEM, jax.ShapeDtypeStruct
        size = hw
        most = max(rows, dim)
        ring = 16 + 2 * SUBS
        sends = 16 * UNITS
        _, _, *results = pl.pallas_call(
            functools.partial(_kernel, n, heads),
            out_shape=[shape((rows, dim), LOW), shape((rows, dim), LOW), shape((tok, dim), LOW), shape((1, dim), F32),
                       shape(wq.shape, LOW), shape(wk.shape, LOW), shape(wv.shape, LOW), shape(wo.shape, LOW)],
            in_specs=[anywhere, anywhere, vmem, anywhere, anywhere, anywhere, anywhere, anywhere, anywhere],
            out_specs=[anywhere, anywhere, anywhere, vmem, anywhere, anywhere, anywhere, anywhere],
            scratch_shapes=[
                scratch(near.shape, F32), scratch(far.shape, F32), scratch((2, tok, dim), LOW), scratch((width, dim), LOW), scratch((most, hw), LOW),
                scratch((n, cols, HEAD), LOW), scratch((most, HEAD), LOW), scratch((HEAD, rows), LOW), scratch((most, HEAD), LOW), scratch((HEAD + 8, rows), LOW),
                scratch((1, cols), F32), scratch((2, cols, HEAD), LOW), scratch((cols // UNITS, HEAD), LOW), scratch((1, cols), F32), scratch((n, 1, cols), F32), scratch((n, HEAD + 8, cols), F32),
                scratch((HEAD, cols), F32), scratch((rows, HEAD), F32), scratch((rows, HEAD), F32), scratch((rows, width), LOW), scratch((width + hw, rows), LOW),
                scratch((4, tok, dim), LOW), scratch((2, half, dim), LOW), scratch((2, 2, half, dim), LOW), scratch((tok, dim), F32),
                scratch((most, size), LOW), scratch((n, 1, dim), F32), scratch((8, dim), F32),
                dma((2, sends)), dma((2, sends)), dma((ring,)), dma((ring,)), dma((n - 1,)), dma((n - 1,)), dma((7,)), dma((dim // hw,)), dma((2, UNITS)), dma((2,)), dma((4 + 2 * SUBS,))],
            compiler_params=pltpu.CompilerParams(collective_id=0, has_side_effects=True, vmem_limit_bytes=VMEM),
            name="layer",
        )(x, dy, gain, wq, wk, wv, wo, near, far)
        kept = [results[i] for i in (2, 3, 4, 0, 5, 1)]
        out = pl.pallas_call(
            _results,
            out_shape=[shape(t.shape, t.dtype) for t in kept],
            in_specs=[anywhere] * len(kept),
            out_specs=[anywhere] * len(kept),
            scratch_shapes=[*[scratch(t.shape, t.dtype) for t in kept], dma((len(kept),)), dma((len(kept),))],
            compiler_params=pltpu.CompilerParams(vmem_limit_bytes=VMEM),
            name="results",
        )(*kept)
        return out[3], out[5], out[0], out[1], out[2], out[4]

    tokens, columns = P(("dp", "tp"), None), P(None, "tp")
    return jax.shard_map(
        step,
        mesh=mesh,
        in_specs=(tokens, tokens, P(None), columns, columns, columns, P("tp", None)),
        out_specs=(tokens, P("dp", None), P("dp", "tp"), P("dp", "tp"), P("dp", "tp"), P(("dp", "tp"), None)),
        check_vma=False,
    )
```
